16 devices in a mesh: batch: 2 (over y, z), dap: 8 (over x, core).
Axes of the slice: x: 4, y: 2, z: 1, core: 2. Of those that a mesh axis runs over, the one named last changes fastest.
The devices are a block of a 4x4x8 slice.
Arguments:
- z_pair: bfloat16 [1024, 512, 64], P(('batch', 'dap')), parts along dimension 0
- pair_mask: int32 [1024, 512], P(('batch', 'dap')), parts along dimension 0
- dz_out: bfloat16 [1024, 512, 64], P(('batch', 'dap')), parts along dimension 0
- ln_in_scale: bfloat16 [64], replicated
- ln_in_offset: bfloat16 [64], replicated
- w_in: bfloat16 [64, 256], replicated
- b_in: bfloat16 [256], replicated
- ln_out_scale: bfloat16 [64], replicated
- ln_out_offset: bfloat16 [64], replicated
- w_out: bfloat16 [64, 64], replicated
- b_out: bfloat16 [64], replicated
- w_gate: bfloat16 [64, 64], replicated
- b_gate: bfloat16 [64], replicated
Outputs:
- output 1: bfloat16 [1024, 512, 64], P(('batch', 'dap')), parts along dimension 0
- output 2: bfloat16 [128], P('batch'), parts along dimension 0
- output 3: bfloat16 [128], P('batch'), parts along dimension 0
- output 4: bfloat16 [128, 256], P('batch'), parts along dimension 0
- output 5: bfloat16 [512], P('batch'), parts along dimension 0
- output 6: bfloat16 [128], P('batch'), parts along dimension 0
- output 7: bfloat16 [128], P('batch'), parts along dimension 0
- output 8: bfloat16 [128, 64], P('batch'), parts along dimension 0
- output 9: bfloat16 [128], P('batch'), parts along dimension 0
- output 10: bfloat16 [128, 64], P('batch'), parts along dimension 0
- output 11: bfloat16 [128], P('batch'), parts along dimension 0
There are 2 independent parts. The reference program is written for one: setup_inputs(seed, part) draws one part's arguments, and reference() takes and returns one part's arrays. A program takes and returns all parts, laid end to end along the dimension named above; an argument that names none is the same for every part.
All inputs are finite; a program needn't handle non-finite values.
Results may differ from the reference program's by a relative error of at most 0.0152256.
Values are sent between devices in bfloat16 or wider.
A program may use at most 768 MiB of HBM per device.

```python
import functools
import jax
import jax.numpy as jnp
from jax import lax

N = 512
CZ = 64
CH = 64
LN_EPS = 1e-5


@jax.custom_vjp
def dense_map(x_act, w_mat):
    return jnp.einsum('...k,km->...m', x_act.astype(jnp.float32), w_mat.astype(jnp.float32))


def dense_fwd(x_act, w_mat):
    return dense_map(x_act, w_mat), (x_act, w_mat)


def dense_bwd(saved_res, grad_out):
    x_act, w_mat = saved_res
    grad_b16 = grad_out.astype(jnp.bfloat16).astype(jnp.float32)
    grad_x = jnp.einsum('...m,km->...k', grad_b16, w_mat.astype(jnp.float32)).astype(jnp.bfloat16)
    grad_w = jnp.einsum('...k,...m->km', x_act.astype(jnp.float32), grad_b16).astype(jnp.bfloat16)
    return grad_x, grad_w


dense_map.defvjp(dense_fwd, dense_bwd)


@jax.custom_vjp
def triangle_map(act_a, act_b):
    return jnp.einsum('ikc,jkc->ijc', act_a.astype(jnp.float32), act_b.astype(jnp.float32))


def triangle_fwd(act_a, act_b):
    return triangle_map(act_a, act_b), (act_a, act_b)


def triangle_bwd(saved_res, grad_out):
    act_a, act_b = saved_res
    grad_b16 = grad_out.astype(jnp.bfloat16).astype(jnp.float32)
    grad_a = jnp.einsum('ijc,jkc->ikc', grad_b16, act_b.astype(jnp.float32)).astype(jnp.bfloat16)
    grad_bb = jnp.einsum('ijc,ikc->jkc', grad_b16, act_a.astype(jnp.float32)).astype(jnp.bfloat16)
    return grad_a, grad_bb


triangle_map.defvjp(triangle_fwd, triangle_bwd)


def layer_norm(x_val, ln_scale, ln_offset):
    mean_val = jnp.mean(x_val, axis=-1, keepdims=True)
    centered = x_val - mean_val
    var_val = jnp.mean(centered * centered, axis=-1, keepdims=True)
    return centered * lax.rsqrt(var_val + LN_EPS) * ln_scale.astype(jnp.float32) + ln_offset.astype(jnp.float32)


def outgoing_layer(z_pair, ln_in_scale, ln_in_offset, w_in, b_in, ln_out_scale, ln_out_offset, w_out, b_out, w_gate, b_gate, pair_mask):
    z_f = z_pair.astype(jnp.float32)
    z_norm = layer_norm(z_f, ln_in_scale, ln_in_offset).astype(jnp.bfloat16)
    w_cat = jnp.concatenate([w_in, w_gate], axis=1)
    b_cat = jnp.concatenate([b_in, b_gate]).astype(jnp.float32)
    proj_all = dense_map(z_norm, w_cat) + b_cat
    mask_f = pair_mask.astype(jnp.float32)[..., None]
    proj_a = proj_all[..., :CH]
    proj_b = proj_all[..., CH:2 * CH]
    sig_a = jax.nn.sigmoid(proj_all[..., 2 * CH:3 * CH])
    sig_b = jax.nn.sigmoid(proj_all[..., 3 * CH:4 * CH])
    sig_g = jax.nn.sigmoid(proj_all[..., 4 * CH:])
    act_a = (mask_f * sig_a * proj_a).astype(jnp.bfloat16)
    act_b = (mask_f * sig_b * proj_b).astype(jnp.bfloat16)
    tri_out = triangle_map(act_a, act_b)
    o_norm = layer_norm(tri_out, ln_out_scale, ln_out_offset).astype(jnp.bfloat16)
    update = (dense_map(o_norm, w_out) + b_out.astype(jnp.float32)).astype(jnp.bfloat16)
    return (z_f + sig_g * update.astype(jnp.float32)).astype(jnp.bfloat16)


def setup_inputs(seed: int = 0, part: int = 0) -> dict:
    part_key = jax.random.fold_in(jax.random.key(seed), part)
    k_z, k_dy, k_res, k_pair = jax.random.split(part_key, 4)
    w_keys = jax.random.split(jax.random.key(seed + 1), 12)
    res_keep = (jax.random.randint(k_res, (N,), 0, 8) != 0).astype(jnp.int32)
    pair_keep = (jax.random.randint(k_pair, (N, N), 0, 16) != 0).astype(jnp.int32)
    pair_mask = res_keep[:, None] * res_keep[None, :] * pair_keep
    return {
        'z_pair': jax.random.normal(k_z, (N, N, CZ), jnp.float32).astype(jnp.bfloat16),
        'pair_mask': pair_mask,
        'dz_out': jax.random.normal(k_dy, (N, N, CZ), jnp.float32).astype(jnp.bfloat16),
        'ln_in_scale': (1.0 + 0.3 * jax.random.normal(w_keys[0], (CZ,), jnp.float32)).astype(jnp.bfloat16),
        'ln_in_offset': (0.3 * jax.random.normal(w_keys[1], (CZ,), jnp.float32)).astype(jnp.bfloat16),
        'w_in': (jax.random.normal(w_keys[2], (CZ, 4 * CH), jnp.float32) * CZ ** -0.5).astype(jnp.bfloat16),
        'b_in': (0.5 * jax.random.normal(w_keys[3], (4 * CH,), jnp.float32)).astype(jnp.bfloat16),
        'ln_out_scale': (1.0 + 0.3 * jax.random.normal(w_keys[4], (CH,), jnp.float32)).astype(jnp.bfloat16),
        'ln_out_offset': (0.3 * jax.random.normal(w_keys[5], (CH,), jnp.float32)).astype(jnp.bfloat16),
        'w_out': (jax.random.normal(w_keys[6], (CH, CZ), jnp.float32) * CH ** -0.5).astype(jnp.bfloat16),
        'b_out': (0.5 * jax.random.normal(w_keys[7], (CZ,), jnp.float32)).astype(jnp.bfloat16),
        'w_gate': (jax.random.normal(w_keys[8], (CZ, CZ), jnp.float32) * CZ ** -0.5).astype(jnp.bfloat16),
        'b_gate': (0.5 * jax.random.normal(w_keys[9], (CZ,), jnp.float32)).astype(jnp.bfloat16),
    }


def reference(z_pair, pair_mask, dz_out, ln_in_scale, ln_in_offset, w_in, b_in, ln_out_scale, ln_out_offset, w_out, b_out, w_gate, b_gate):
    layer_fn = functools.partial(outgoing_layer, pair_mask=pair_mask)
    z_next, vjp_fn = jax.vjp(layer_fn, z_pair, ln_in_scale, ln_in_offset, w_in, b_in, ln_out_scale, ln_out_offset, w_out, b_out, w_gate, b_gate)
    d_z, d_in_scale, d_in_offset, d_w_in, d_b_in, d_out_scale, d_out_offset, d_w_out, d_b_out, d_w_gate, d_b_gate = vjp_fn(dz_out)
    return (d_z, d_in_scale, d_in_offset, d_w_in, d_b_in, d_out_scale, d_out_offset, d_w_out, d_b_out, d_w_gate, d_b_gate)
```

```python
import functools
import jax
import jax.numpy as jnp
from jax import lax
from jax.experimental import pallas as pl
from jax.experimental.pallas import tpu as pltpu
from jax.sharding import PartitionSpec as P

LN_EPS = 1e-5
F32 = jnp.float32
BF16 = jnp.bfloat16
SUB = 8
VMEM_LIMIT = 63 * 1024 * 1024


def nn_dot(lhs, rhs):
    return lax.dot_general(lhs, rhs, (((1,), (0,)), ((), ())), preferred_element_type=F32)


def nt_dot(lhs, rhs):
    return lax.dot_general(lhs, rhs, (((1,), (1,)), ((), ())), preferred_element_type=F32)


def tn_dot(lhs, rhs):
    return lax.dot_general(lhs, rhs, (((0,), (0,)), ((), ())), preferred_element_type=F32)


def row_norm(z8, scale, offset):
    mean_val = jnp.mean(z8, axis=1, keepdims=True)
    centered = z8 - mean_val
    inv_std = lax.rsqrt(jnp.mean(centered * centered, axis=1, keepdims=True) + LN_EPS)
    z_hat = centered * inv_std
    return z_hat, inv_std, (z_hat * scale[None] + offset[None]).astype(BF16)


def lanes(bias, width):
    return jnp.concatenate([bias] * (width // bias.shape[-1]), axis=-1)


def gated(prod, bias_ref, start, chans, mask_half):
    cols = prod.shape[-1]
    val = prod[:chans * SUB].reshape(chans, SUB, cols) + lanes(bias_ref[start:start + chans], cols)
    gate = prod[chans * SUB:].reshape(chans, SUB, cols) + lanes(bias_ref[start + chans:start + 2 * chans], cols)
    return (jnp.tanh(gate) + 1.0) * (val * mask_half[None])


def own_kernel(z_ref, dy_ref, mask_ref, wk_ref, bias_ref, gk_ref, gbias_ref, perm_ref, sc_ref, off_ref, a_ref, lg_ref, dyt_ref):
    chans = a_ref.shape[0]
    cols = z_ref.shape[-1]
    a_parts, dy_parts = [], []
    for half in range(2):
        rows = slice(half * SUB, (half + 1) * SUB)
        _, _, zn = row_norm(z_ref[rows].astype(F32), sc_ref[...], off_ref[...])
        zn2 = zn.reshape(SUB * zn.shape[1], cols)
        mask_half = mask_ref[rows].astype(F32) * 0.5
        a_parts.append(gated(nn_dot(wk_ref[...], zn2), bias_ref, 0, chans, mask_half))
        lg = nn_dot(gk_ref[...], zn2).reshape(chans, SUB, cols) + lanes(gbias_ref[...], cols)
        lg_ref[:, rows, :] = lg
        dy2 = dy_ref[rows].reshape(SUB * dy_ref.shape[1], cols)
        dy_parts.append(nn_dot(perm_ref[...], dy2).reshape(chans, SUB, cols))
    a_ref[...] = jnp.concatenate(a_parts, axis=1).astype(BF16)
    dyt_ref[...] = jnp.concatenate(dy_parts, axis=1).astype(BF16)


def all_kernel(*refs):
    z_ref, mask_ref, wka_ref, wkb_ref, ba_ref, bb_ref, sc_ref, off_ref = refs[:8]
    a_ref, b_ref = refs[-2:]
    cols = z_ref.shape[-1]
    a_parts, b_parts = [], []
    for half in range(2):
        rows = slice(half * SUB, (half + 1) * SUB)
        _, _, zn = row_norm(z_ref[0, rows].astype(F32), sc_ref[...], off_ref[...])
        zn2 = zn.reshape(SUB * zn.shape[1], cols)
        mask_half = mask_ref[0, rows].astype(F32) * 0.5
        a_parts.append(gated(nn_dot(wka_ref[...], zn2), ba_ref, 0, a_ref.shape[0], mask_half))
        b_parts.append(gated(nn_dot(wkb_ref[...], zn2), bb_ref, 0, b_ref.shape[0], mask_half))
    a_ref[...] = jnp.concatenate(a_parts, axis=1).astype(BF16)
    b_ref[...] = jnp.concatenate(b_parts, axis=1).astype(BF16)


def chain_kernel(a_ref, b_ref, lg_ref, dyt_ref, wo_ref, wot_ref, bout_ref, sc_ref, off_ref,
                 do_ref, dgl_ref, da_ref, gram_ref, dbg_ref, dbo_ref, dsc_ref, dof_ref, o_s, da_s):
    chans, rows, _ = a_ref.shape
    jb = b_ref.shape[1]
    step = pl.program_id(0)

    @pl.when(step == 0)
    def _():
        da_s[...] = jnp.zeros_like(da_s)
        for ref in (gram_ref, dbg_ref, dbo_ref, dsc_ref, dof_ref):
            ref[...] = jnp.zeros_like(ref)

    def o_body(c, carry):
        o_s[c] = nt_dot(a_ref[c], b_ref[c])
        return carry
    lax.fori_loop(0, chans, o_body, 0, unroll=4)

    def chain_body(g, carry):
        dgl_parts, dt_parts = [], []
        for half in range(2):
            r0 = pl.multiple_of(g * 2 * SUB + half * SUB, SUB)
            o8 = o_s[:, pl.ds(r0, SUB), :]
            centered = o8 - jnp.mean(o8, axis=0, keepdims=True)
            inv_std = lax.rsqrt(jnp.mean(centered * centered, axis=0, keepdims=True) + LN_EPS)
            o_hat = centered * inv_std
            o_norm = (o_hat * sc_ref[...] + off_ref[...]).astype(BF16).reshape(chans * SUB, jb)
            upd = (nn_dot(wo_ref[...], o_norm).reshape(chans, SUB, jb) + bout_ref[...]).astype(BF16).astype(F32)
            sig = jnp.tanh(lg_ref[:, pl.ds(r0, SUB), :] * 0.5) * 0.5 + 0.5
            dyf = dyt_ref[:, pl.ds(pl.multiple_of(g * 2 * SUB, 2 * SUB), 2 * SUB), :].astype(F32)[:, half * SUB:(half + 1) * SUB]
            prod = sig * dyf
            d_upd = prod.astype(BF16)
            dgl = prod * upd * (1.0 - sig)
            dbg_ref[...] += dgl
            dgl_parts.append(dgl)
            dbo_ref[...] += d_upd.astype(F32)
            d_upd2 = d_upd.reshape(chans * SUB, jb)
            gram_ref[...] += nt_dot(o_norm, d_upd2)
            d_on = nn_dot(wot_ref[...], d_upd2).astype(BF16).astype(F32).reshape(chans, SUB, jb)
            dsc_ref[...] += d_on * o_hat
            dof_ref[...] += d_on
            g_hat = d_on * sc_ref[...]
            m1 = jnp.mean(g_hat, axis=0, keepdims=True)
            m2 = jnp.mean(g_hat * o_hat, axis=0, keepdims=True)
            dt_parts.append(inv_std * (g_hat - m1 - o_hat * m2))
        pair = pl.ds(pl.multiple_of(g * 2 * SUB, 2 * SUB), 2 * SUB)
        dgl_ref[:, pair, :] = jnp.concatenate(dgl_parts, axis=1).astype(BF16)
        do_ref[0, :, pair, :] = jnp.concatenate(dt_parts, axis=1).astype(BF16)
        return carry
    lax.fori_loop(0, rows // (2 * SUB), chain_body, 0)

    def da_body(c, carry):
        da_s[c] += nn_dot(do_ref[0, c], b_ref[c])
        return carry
    lax.fori_loop(0, chans, da_body, 0, unroll=4)

    @pl.when(step == pl.num_programs(0) - 1)
    def _():
        da_ref[...] = da_s[...].astype(BF16)


def db_kernel(do_ref, a_ref, db_ref):
    per = do_ref.shape[1]
    for c in range(per):
        lhs = do_ref[:, c].reshape(do_ref.shape[0] * do_ref.shape[2], do_ref.shape[3])
        db_ref[c] = tn_dot(lhs, a_ref[c]).astype(BF16)


def input_kernel(z_ref, dy_ref, mask_ref, da_ref, db_ref, dgl_ref, wk_ref, bias_ref, wg_ref, sc_ref, off_ref,
                 dz_ref, gram_ref, dbias_ref, dsc_ref, dof_ref, dp_s):
    chans = da_ref.shape[0]
    chan_z, cols = z_ref.shape[1:]

    @pl.when(pl.program_id(0) == 0)
    def _():
        for ref in (gram_ref, dbias_ref, dsc_ref, dof_ref):
            ref[...] = jnp.zeros_like(ref)

    def fold(val):
        acc = val[..., :128]
        for lane in range(128, cols, 128):
            acc = acc + val[..., lane:lane + 128]
        return acc

    n_p = chans * SUB
    for half in range(2):
        rows = slice(half * SUB, (half + 1) * SUB)
        z_hat, inv_std, zn = row_norm(z_ref[rows].astype(F32), sc_ref[...], off_ref[...])
        zn2 = zn.reshape(SUB * chan_z, cols)
        mask_f = mask_ref[rows].astype(F32)[None]
        for side, grad_ref in enumerate((da_ref, db_ref)):
            prod = nn_dot(wk_ref[side * 2 * n_p:(side + 1) * 2 * n_p], zn2)
            val = prod[:n_p].reshape(chans, SUB, cols) + lanes(bias_ref[side * 2 * chans:side * 2 * chans + chans], cols)
            gate = prod[n_p:].reshape(chans, SUB, cols) + lanes(bias_ref[side * 2 * chans + chans:(side + 1) * 2 * chans], cols)
            sig = jnp.tanh(gate) * 0.5 + 0.5
            grad = grad_ref[...].astype(F32)[:, rows] * mask_f
            d_val = grad * sig
            d_gate = d_val * val * (1.0 - sig)
            dbias_ref[side * chans:(side + 1) * chans] += fold(d_val)
            dbias_ref[(side + 2) * chans:(side + 3) * chans] += fold(d_gate)
            dp_s[side * n_p:(side + 1) * n_p] = d_val.astype(BF16).reshape(n_p, cols)
            dp_s[(side + 2) * n_p:(side + 3) * n_p] = d_gate.astype(BF16).reshape(n_p, cols)
        dp_s[4 * n_p:] = dgl_ref[...].astype(F32)[:, rows].astype(BF16).reshape(n_p, cols)
        d_zn = nn_dot(wg_ref[...], dp_s[...]).astype(BF16).astype(F32).reshape(SUB, chan_z, cols)
        gram = nt_dot(zn2, dp_s[...]).reshape(SUB, chan_z, dp_s.shape[0])
        lane_row = lax.broadcasted_iota(jnp.int32, (chan_z, dp_s.shape[0]), 1) % SUB
        acc = gram_ref[...]
        for i in range(SUB):
            acc = acc + jnp.where(lane_row == i, gram[i], 0.0)
        gram_ref[...] = acc
        dsc_ref[...] += jnp.sum(d_zn * z_hat, axis=0)
        dof_ref[...] += jnp.sum(d_zn, axis=0)
        g_hat = d_zn * sc_ref[...][None]
        m1 = jnp.mean(g_hat, axis=1, keepdims=True)
        m2 = jnp.mean(g_hat * z_hat, axis=1, keepdims=True)
        d_z = dy_ref[rows].astype(F32) + inv_std * (g_hat - m1 - z_hat * m2)
        dz_ref[rows] = d_z.astype(BF16)


def spread(w_t):
    eye = jnp.eye(SUB, dtype=w_t.dtype)
    return (w_t[:, None, None, :] * eye[None, :, :, None]).reshape(w_t.shape[0] * SUB, SUB * w_t.shape[1])


def same_rows(w_t):
    eye = jnp.eye(SUB, dtype=w_t.dtype)
    return (w_t[:, None, :, None] * eye[None, :, None, :]).reshape(w_t.shape[0] * SUB, SUB * w_t.shape[1])


def vec8(vec):
    return jnp.broadcast_to(vec.astype(F32)[:, None, None], (vec.shape[0], SUB, 128))


def whole(arr):
    nd = arr.ndim
    return pl.BlockSpec(arr.shape, lambda *_: (0,) * nd, pipeline_mode=pl.Buffered(1))


def params(**kw):
    return pltpu.CompilerParams(vmem_limit_bytes=VMEM_LIMIT, **kw)


def local_grads(n_dap, z_loc, mask_loc, dy_loc, ln_in_scale, ln_in_offset, w_in, b_in, ln_out_scale, ln_out_offset, w_out, b_out, w_gate, b_gate):
    rows, cols, cz = z_loc.shape
    ch = w_in.shape[1] // 4
    half = ch // 2
    total = rows * n_dap
    jb = 2 * rows
    sds = jax.ShapeDtypeStruct
    core = lax.axis_index('dap') % 2
    z_t = jnp.transpose(z_loc, (0, 2, 1))
    dy_t = jnp.transpose(dy_loc, (0, 2, 1))

    w_t = w_in.T
    w_pa, w_pb, w_la, w_lb = w_t[:ch], w_t[ch:2 * ch], w_t[2 * ch:3 * ch] * 0.5, w_t[3 * ch:] * 0.5
    b_pa, b_pb, b_la, b_lb = b_in[:ch], b_in[ch:2 * ch], b_in[2 * ch:3 * ch] * 0.5, b_in[3 * ch:] * 0.5
    mine = lambda arr: lax.dynamic_slice_in_dim(arr, core * half, half, 0)
    wk_a = spread(jnp.concatenate([w_pa, w_la]))
    wk_b = spread(jnp.concatenate([w_pb, w_lb]))
    wk_ah = spread(jnp.concatenate([mine(w_pa), mine(w_la)]))
    bias_a = vec8(jnp.concatenate([b_pa, b_la]))
    bias_b = vec8(jnp.concatenate([b_pb, b_lb]))
    bias_ah = vec8(jnp.concatenate([mine(b_pa), mine(b_la)]))
    sc_in = jnp.broadcast_to(ln_in_scale.astype(F32)[:, None], (cz, cols))
    off_in = jnp.broadcast_to(ln_in_offset.astype(F32)[:, None], (cz, cols))
    gk = spread(w_gate.T)
    perm = spread(jnp.eye(cz, dtype=BF16))

    grp = 2 * SUB
    n_grp = rows // grp
    chunks = []
    for q in range(n_grp):
        piece = z_t[q * grp:(q + 1) * grp]
        if q == 0:
            piece = jnp.concatenate([piece, mask_loc.astype(BF16).reshape(rows // cz, cz, cols)], axis=0)
        chunks.append(lax.all_gather(piece, 'dap', axis=0))
    mask_all = chunks[0][:, grp:].reshape(n_dap, rows, cols)

    row3 = lambda nd: pl.BlockSpec((grp, nd, cols), lambda g: (g, 0, 0))
    chan_rows = lambda n: pl.BlockSpec((n, grp, cols), lambda g: (0, g, 0))
    mask_spec = pl.BlockSpec((grp, cols), lambda g: (g, 0))
    args = (z_t, dy_t, mask_loc, wk_a, bias_a, gk, vec8(b_gate), perm, sc_in, off_in)
    a_own, lg, dyt = pl.pallas_call(
        own_kernel, grid=(n_grp,), name='own_rows',
        out_shape=(sds((ch, rows, cols), BF16), sds((cz, rows, cols), F32), sds((cz, rows, cols), BF16)),
        in_specs=[row3(cz), row3(cz), mask_spec] + [whole(x) for x in args[3:]],
        out_specs=(chan_rows(ch), chan_rows(cz), chan_rows(cz)),
        cost_estimate=pl.CostEstimate(flops=10**10, bytes_accessed=30 * 2**20, transcendentals=0),
        compiler_params=params())(*args)

    a_half = b_full = None
    for q in range(n_grp):
        args = (chunks[q], mask_all, wk_ah, wk_b, bias_ah, bias_b, sc_in, off_in)
        specs = [pl.BlockSpec((1, grp, cz, cols), lambda p: (p, 0, 0, 0)),
                 pl.BlockSpec((1, grp, cols), lambda p, q=q: (p, q, 0))] + [whole(x) for x in args[2:]]
        alias = {}
        if q:
            args = args + (a_half, b_full)
            specs = specs + [pl.BlockSpec(memory_space=pl.ANY)] * 2
            alias = {8: 0, 9: 1}
        a_half, b_full = pl.pallas_call(
            all_kernel, grid=(n_dap,), name=f'all_rows_{q}',
            out_shape=(sds((half, total, cols), BF16), sds((ch, total, cols), BF16)),
            in_specs=specs,
            out_specs=(pl.BlockSpec((half, grp, cols), lambda p, q=q: (0, p * n_grp + q, 0)),
                       pl.BlockSpec((ch, grp, cols), lambda p, q=q: (0, p * n_grp + q, 0))),
            input_output_aliases=alias,
            cost_estimate=pl.CostEstimate(flops=2 * 10**10, bytes_accessed=30 * 2**20, transcendentals=0),
            compiler_params=params())(*args)

    sc_out, off_out = vec8(ln_out_scale), vec8(ln_out_offset)
    args = (a_own, b_full, lg, dyt, same_rows(w_out.T), same_rows(w_out), vec8(b_out), sc_out, off_out)
    acc_shape = sds((ch, SUB, 128), F32)
    acc_spec = pl.BlockSpec((ch, SUB, 128), lambda j: (0, 0, 0))
    col_spec = pl.BlockSpec((ch, rows, jb), lambda j: (0, 0, j))
    gram_n = ch * SUB
    do_blk, dgl, da, gram_o, dbg, dbo, dsc_o, dof_o = pl.pallas_call(
        chain_kernel, grid=(total // jb,), name='chain',
        out_shape=(sds((total // jb, ch, rows, jb), BF16), sds((cz, rows, cols), BF16), sds((ch, rows, cols), BF16),
                   sds((gram_n, gram_n), F32), acc_shape, acc_shape, acc_shape, acc_shape),
        in_specs=[whole(a_own), pl.BlockSpec((ch, jb, cols), lambda j: (0, j, 0)), col_spec, col_spec] + [whole(x) for x in args[4:]],
        out_specs=(pl.BlockSpec((1, ch, rows, jb), lambda j: (j, 0, 0, 0)), col_spec,
                   pl.BlockSpec((ch, rows, cols), lambda j: (0, 0, 0), pipeline_mode=pl.Buffered(1)),
                   pl.BlockSpec((gram_n, gram_n), lambda j: (0, 0)), acc_spec, acc_spec, acc_spec, acc_spec),
        scratch_shapes=[pltpu.VMEM((ch, rows, jb), F32), pltpu.VMEM((ch, rows, cols), F32)],
        cost_estimate=pl.CostEstimate(flops=2 * 10**10, bytes_accessed=60 * 2**20, transcendentals=0),
        compiler_params=params())(*args)

    do_all = lax.all_to_all(do_blk.reshape(n_dap, half, rows, jb), 'dap', 0, 0)
    per = 4
    db_pair = pl.pallas_call(
        db_kernel, grid=(half // per,), name='db',
        out_shape=sds((half, jb, cols), BF16),
        in_specs=[pl.BlockSpec((n_dap, per, rows, jb), lambda c: (0, c, 0, 0)),
                  pl.BlockSpec((per, total, cols), lambda c: (c, 0, 0))],
        out_specs=pl.BlockSpec((per, jb, cols), lambda c: (c, 0, 0)),
        cost_estimate=pl.CostEstimate(flops=10**10, bytes_accessed=30 * 2**20, transcendentals=0),
        compiler_params=params())(do_all, a_half)
    keep = lax.dynamic_slice_in_dim(db_pair, core * rows, rows, 1)
    give = lax.dynamic_slice_in_dim(db_pair, (1 - core) * rows, rows, 1)
    got = lax.ppermute(give, 'dap', [(i, i ^ 1) for i in range(n_dap)])
    low = core == 0
    db = jnp.concatenate([jnp.where(low, keep, got), jnp.where(low, got, keep)], axis=0)

    w_back = jnp.concatenate([w_in, w_gate], axis=1)
    eye = jnp.eye(SUB, dtype=BF16)
    wg = (w_back[None, :, :, None] * eye[:, None, None, :]).reshape(SUB * cz, w_back.shape[1] * SUB)
    args = (z_t, dy_t, mask_loc, da, db, dgl, jnp.concatenate([wk_a, wk_b]), jnp.concatenate([bias_a, bias_b]), wg, sc_in, off_in)
    n_e = w_back.shape[1]
    const = lambda *shape: pl.BlockSpec(shape, lambda g: (0,) * len(shape))
    dz_t, gram_i, dbias, dsc_i, dof_i = pl.pallas_call(
        input_kernel, grid=(n_grp,), name='input_side',
        out_shape=(sds((rows, cz, cols), BF16), sds((cz, n_e * SUB), F32), sds((4 * ch, SUB, 128), F32),
                   sds((cz, cols), F32), sds((cz, cols), F32)),
        in_specs=[row3(cz), row3(cz), mask_spec, chan_rows(ch), chan_rows(ch), chan_rows(cz)] + [whole(x) for x in args[6:]],
        out_specs=(row3(cz), const(cz, n_e * SUB), const(4 * ch, SUB, 128), const(cz, cols), const(cz, cols)),
        scratch_shapes=[pltpu.VMEM((n_e * SUB, cols), BF16)],
        cost_estimate=pl.CostEstimate(flops=10**10, bytes_accessed=30 * 2**20, transcendentals=0),
        compiler_params=params())(*args)

    d_w = gram_i.reshape(cz, n_e, SUB).sum(-1)
    d_wout = jnp.einsum('cidi->cd', gram_o.reshape(ch, SUB, cz, SUB))
    tail = lambda acc: acc.sum((-2, -1))
    partial = (dsc_i.sum(-1), dof_i.sum(-1), d_w[:, :4 * ch], tail(dbias), tail(dsc_o), tail(dof_o), d_wout, tail(dbo), d_w[:, 4 * ch:], tail(dbg))
    summed = lax.psum(partial, 'dap')
    return (jnp.transpose(dz_t, (0, 2, 1)),) + tuple(piece.astype(BF16) for piece in summed)


def solution(mesh):
    pair_spec = P(('batch', 'dap'), None, None)
    mask_spec = P(('batch', 'dap'), None)
    vec_rep = P(None)
    mat_rep = P(None, None)
    vec_part = P('batch')
    mat_part = P('batch', None)
    in_specs = (pair_spec, mask_spec, pair_spec, vec_rep, vec_rep, mat_rep, vec_rep, vec_rep, vec_rep, mat_rep, vec_rep, mat_rep, vec_rep)
    out_specs = (pair_spec, vec_part, vec_part, mat_part, vec_part, vec_part, vec_part, mat_part, vec_part, mat_part, vec_part)
    body = functools.partial(local_grads, mesh.shape['dap'])
    return jax.shard_map(body, mesh=mesh, in_specs=in_specs, out_specs=out_specs, check_vma=False)
```

```python
import functools
import jax
import jax.numpy as jnp
from jax import lax
from jax.experimental import pallas as pl
from jax.experimental.pallas import tpu as pltpu
from jax.sharding import PartitionSpec as P

LN_EPS = 1e-5
F32 = jnp.float32
BF16 = jnp.bfloat16
SUB = 8
VMEM_LIMIT = 63 * 1024 * 1024
COST = 5e8


def nn_dot(lhs, rhs):
    return lax.dot_general(lhs, rhs, (((1,), (0,)), ((), ())), preferred_element_type=F32)


def nt_dot(lhs, rhs):
    return lax.dot_general(lhs, rhs, (((1,), (1,)), ((), ())), preferred_element_type=F32)


def tn_dot(lhs, rhs):
    return lax.dot_general(lhs, rhs, (((0,), (0,)), ((), ())), preferred_element_type=F32)


def row_norm(z8, scale, offset):
    mean_val = jnp.mean(z8, axis=1, keepdims=True)
    centered = z8 - mean_val
    inv_std = lax.rsqrt(jnp.mean(centered * centered, axis=1, keepdims=True) + LN_EPS)
    z_hat = centered * inv_std
    return z_hat, inv_std, (z_hat * scale[None] + offset[None]).astype(BF16)


def lanes(bias, width):
    return jnp.concatenate([bias] * (width // bias.shape[-1]), axis=-1)


def gated(prod, bias_ref, start, chans, mask_half):
    cols = prod.shape[-1]
    val = prod[:chans * SUB].reshape(chans, SUB, cols) + lanes(bias_ref[start:start + chans], cols)
    gate = prod[chans * SUB:].reshape(chans, SUB, cols) + lanes(bias_ref[start + chans:start + 2 * chans], cols)
    return (jnp.tanh(gate) + 1.0) * (val * mask_half[None])


def build_weights(core, w_in, w_out, w_gate, vecs, wk_ref, wg_ref, bias_ref, sc_ref, off_ref, perm_s, wok_s, wotk_s, bo_s, osc_s, ooff_s):
    cz = w_in.shape[0]
    ch = w_in.shape[1] // 4
    big = ch * SUB

    def iota(shape, dim):
        return lax.broadcasted_iota(jnp.int32, shape, dim)

    def one(cond):
        return jnp.where(cond, 1.0, 0.0).astype(BF16)

    turn = core * (ch // 2)
    rep = iota((big, ch), 0) // SUB == iota((big, ch), 1)
    rep_c = lax.rem(iota((big, ch), 0) // SUB + turn, ch) == iota((big, ch), 1)
    rep_t = iota((ch, big), 1) // SUB == iota((ch, big), 0)
    rep_ct = lax.rem(iota((ch, big), 1) // SUB + turn, ch) == iota((ch, big), 0)
    tile = one(iota((cz, SUB * cz), 1) % cz == iota((cz, SUB * cz), 0))
    tile_t = one(iota((SUB * cz, cz), 0) % cz == iota((SUB * cz, cz), 1))
    keep = iota((big, SUB * cz), 0) % SUB == iota((big, SUB * cz), 1) // cz
    keep_t = iota((SUB * cz, big), 1) % SUB == iota((SUB * cz, big), 0) // cz
    same = iota((big, big), 0) % SUB == iota((big, big), 1) % SUB

    def spread(wide):
        return jnp.where(keep, nn_dot(wide, tile), 0.0).astype(BF16)

    def column(sel, row, width):
        picked = jnp.where(sel, jnp.broadcast_to(row.astype(F32), sel.shape), 0.0).astype(BF16)
        return nn_dot(picked, jnp.ones((sel.shape[1], width), BF16))

    def eights(sel, row):
        return column(sel, row, 128).reshape(ch, SUB, 128)

    for dst, src, scale in ((0, 0, 1.0), (1, 2, 0.5), (2, 1, 1.0), (3, 3, 0.5), (4, None, 1.0)):
        w_part = w_gate[...] if src is None else w_in[:, src * ch:(src + 1) * ch]
        sel, sel_t = (rep, rep_t) if src is None else (rep_c, rep_ct)
        at = slice(dst * big, (dst + 1) * big)
        wide = (nt_dot(one(sel), w_part) * scale).astype(BF16)
        wk_ref[at] = spread(wide)
        wg_ref[:, at] = jnp.where(keep_t, nn_dot(tile_t, nn_dot(w_part, one(sel_t)).astype(BF16)), 0.0).astype(BF16)
        vec = 5 if src is None else 6 + src
        bias_ref[dst * ch:(dst + 1) * ch] = eights(sel, vecs[vec:vec + 1]) * scale
    eye = iota((cz, cz), 0) == iota((cz, cz), 1)
    perm_s[...] = spread(one(rep))
    wok_s[...] = jnp.where(same, nn_dot(nt_dot(one(rep), w_out[...]).astype(BF16), one(rep_ct)), 0.0).astype(BF16)
    wotk_s[...] = jnp.where(same, nn_dot(nn_dot(one(rep_c), w_out[...]).astype(BF16), one(rep_t)), 0.0).astype(BF16)
    sc_ref[...] = column(eye, vecs[0:1], sc_ref.shape[1])
    off_ref[...] = column(eye, vecs[1:2], off_ref.shape[1])
    osc_s[...] = eights(rep_c, vecs[2:3])
    ooff_s[...] = eights(rep_c, vecs[3:4])
    bo_s[...] = eights(rep, vecs[4:5])


def project(z8, mask_half, wk_ref, bias_ref, sc_ref, off_ref, chans):
    cols = z8.shape[-1]
    _, _, zn = row_norm(z8.astype(F32), sc_ref[...], off_ref[...])
    zn2 = zn.reshape(SUB * zn.shape[1], cols)
    n_p = 2 * chans * SUB
    act_a = gated(nn_dot(wk_ref[:n_p], zn2), bias_ref, 0, chans, mask_half)
    act_b = gated(nn_dot(wk_ref[n_p:2 * n_p], zn2), bias_ref, 2 * chans, chans, mask_half)
    return act_a, act_b, zn2


MESH = pl.DeviceIdType.MESH
OWN, LEFT, RIGHT, OPP = range(4)
HOPS = (0, -1, 1, 2)


def blk(shape, index_map):
    return pl.BlockSpec(shape, index_map)


def front_kernel(n_dap, z_own, dy_ref, m_own, w_in, w_out, w_gate, vecs,
                 da_ref, keep_ref, got_ref, dgl_ref, gram_ref, dbg_ref, dbo_ref, dsc_ref, dof_ref, wk_ref, wg_ref, bias_ref, sc_ref, off_ref,
                 give_ref, z_far, m_far, a_all, b_pair, a_sib, lg_ref, dyt_ref, do_out, do_in,
                 perm_ref, wo_ref, wot_ref, bout_ref, osc_ref, ooff_ref,
                 o_s, gram_s, lg_v, dyt_v, do_v, dgl_v, send_sem, recv_sem, loc_sem):
    n_chip = n_dap // 2
    _, rows, cz, cols = z_own.shape
    z_ref, mask_ref = z_own.at[0], m_own.at[0]
    chans = a_all.shape[1]
    half = chans // 2
    hr = rows // 2
    jb = 2 * rows
    grp = 2 * SUB
    me = lax.axis_index('dap')
    core, chip = lax.rem(me, 2), me // 2
    low = core == 0

    def peer(hop, flip):
        to = lax.rem(chip + (hop + n_chip), n_chip) * 2
        return {'dap': to + (1 - core if flip else core)}

    def copy(k, src, dst, hop, flip):
        return pltpu.make_async_remote_copy(src_ref=src, dst_ref=dst, send_sem=send_sem.at[k], recv_sem=recv_sem.at[k],
                                            device_id=peer(hop, flip), device_id_type=MESH)

    barrier = pltpu.get_barrier_semaphore()
    for hop in HOPS:
        for flip in (0, 1):
            if hop or flip:
                pl.semaphore_signal(barrier, inc=1, device_id=peer(hop, flip), device_id_type=MESH)
    pl.semaphore_wait(barrier, n_dap - 1)

    n_grp = rows // grp
    masks = [copy(i, mask_ref, m_far.at[i], hop, 0) for i, hop in enumerate((1, -1, 2))]
    quarter = lambda q: pl.ds(pl.multiple_of(q * grp, grp), grp)
    z_r = lambda q: copy(3 + q, z_ref.at[quarter(q)], z_far.at[0, quarter(q)], 1, 0)
    z_l = lambda q: copy(3 + n_grp + q, z_ref.at[quarter(q)], z_far.at[1, quarter(q)], -1, 0)
    fwd_r = lambda q: copy(3 + 2 * n_grp + q, z_far.at[0, quarter(q)], z_far.at[2, quarter(q)], 1, 0)
    fwd_l = lambda q: copy(3 + 2 * n_grp + q, z_far.at[1, quarter(q)], z_far.at[2, quarter(q)], -1, 0)
    base_b = 3 + 3 * n_grp
    my_rows = pl.multiple_of(core * rows, rows)

    def swap_b(r, q):
        at = pl.ds(pl.multiple_of(my_rows + q * grp, grp), grp)
        return [copy(base_b + (r * n_grp + q) * 2 + h, b_pair.at[r, pl.ds(h * half, half), at], b_pair.at[r, pl.ds((1 - h) * half, half), at], 0, 1) for h in (0, 1)]

    base_a = base_b + 8 * n_grp
    swap_a = lambda r, q: copy(base_a + r * n_grp + q, a_all.at[r, pl.ds(half, half), quarter(q)], a_sib.at[r, :, quarter(q)], 0, 1)
    base_s = base_a + 4 * n_grp
    back = (OWN, RIGHT, LEFT, OPP)
    ship = [[None if (r == OWN and side == 0) else
             copy(base_s + 2 * r + side, do_out.at[r, pl.ds(side * half, half)], do_in.at[back[r], side], HOPS[r], side) for side in (0, 1)] for r in range(4)]
    swap_d = [copy(base_s + 8 + q, give_ref.at[pl.ds(q * (half // 2), half // 2)], got_ref.at[pl.ds(q * (half // 2), half // 2)], 0, 1) for q in (0, 1)]

    for c in masks:
        c.start()
    for q in range(n_grp):
        z_r(q).start()
        z_l(n_grp - 1 - q).start()
    build_weights(core, w_in, w_out, w_gate, vecs, wk_ref, wg_ref, bias_ref, sc_ref, off_ref, perm_ref, wo_ref, wot_ref, bout_ref, osc_ref, ooff_ref)

    row3 = blk((grp, cz, cols), lambda g: (g, 0, 0))
    row2 = blk((grp, cols), lambda g: (g, 0))
    chan3 = lambda n: blk((n, grp, cols), lambda g: (0, g, 0))

    def ab_body(z_b, m_b, a_b, b_b):
        a_parts, b_parts = [], []
        for h in range(2):
            rws = slice(h * SUB, (h + 1) * SUB)
            act_a, act_b, _ = project(z_b[0, rws], m_b[0, rws].astype(F32) * 0.5, wk_ref, bias_ref, sc_ref, off_ref, chans)
            a_parts.append(act_a)
            b_parts.append(act_b)
        a_b[0] = jnp.concatenate(a_parts, axis=1).astype(BF16)
        b_b[0] = jnp.concatenate(b_parts, axis=1).astype(BF16)

    def project_rows(z_src, m_src, n, slot, place):
        pltpu.emit_pipeline(
            ab_body, grid=(n,),
            in_specs=[blk((1, grp, cz, cols), lambda g: (slot(g), place(g)[1], 0, 0)), blk((1, grp, cols), lambda g: (slot(g), place(g)[1], 0))],
            out_specs=[blk((1, chans, grp, cols), lambda g: (place(g)[0], 0, place(g)[1], 0)),
                       blk((1, chans, grp, cols), lambda g: (place(g)[0], 0, core * n_grp + place(g)[1], 0))])(z_src, m_src, a_all, b_pair)

    def swap(r, q):
        for c in swap_b(r, q):
            c.start()
        swap_a(r, q).start()

    def swapped_b(r):
        def body(q, carry):
            for c in swap_b(r, q):
                c.wait_recv()
            return carry
        lax.fori_loop(0, n_grp, body, 0)

    def lg_body(z_b, dy_b, lg_b, dyt_b):
        dy_parts = []
        for h in range(2):
            rws = slice(h * SUB, (h + 1) * SUB)
            _, _, zn = row_norm(z_b[rws].astype(F32), sc_ref[...], off_ref[...])
            zn2 = zn.reshape(SUB * cz, cols)
            lg_b[:, rws, :] = nn_dot(wk_ref[4 * chans * SUB:], zn2).reshape(cz, SUB, cols) + lanes(bias_ref[4 * chans:], cols)
            dy_parts.append(nn_dot(perm_ref[...], dy_b[rws].reshape(SUB * cz, cols)).reshape(cz, SUB, cols))
        dyt_b[...] = jnp.concatenate(dy_parts, axis=1).astype(BF16)

    for ref in (dbg_ref, dbo_ref, dsc_ref, dof_ref, gram_s):
        ref[...] = jnp.zeros_like(ref)

    per = chans // 8

    def o_body(a_b, b_b):
        base = pl.program_id(0) * per
        for c in range(per):
            o_s[base + c] = nt_dot(a_b[c], b_b[c])

    def chain(r):
        where = lax.rem(chip + (HOPS[r] + n_chip), n_chip)
        col = pl.ds(pl.multiple_of(where * jb, jb), jb)
        get_lg = pltpu.make_async_copy(lg_ref.at[:, :, col], lg_v, loc_sem.at[0])
        get_dy = pltpu.make_async_copy(dyt_ref.at[:, :, col], dyt_v, loc_sem.at[1])
        get_lg.start()
        get_dy.start()
        pltpu.emit_pipeline(o_body, grid=(8,), in_specs=[blk((per, rows, cols), lambda s: (s, 0, 0)), blk((per, jb, cols), lambda s: (s, 0, 0))])(
            a_all.at[OWN], b_pair.at[r])
        get_lg.wait()
        get_dy.wait()

        def chain_body(g, carry):
            pair = pl.ds(pl.multiple_of(g * 2 * SUB, 2 * SUB), 2 * SUB)

            def wide(ref):
                val = ref[:, pair, :].astype(F32)
                return jnp.concatenate([val[:, :SUB], val[:, SUB:]], axis=2)

            def tall(val):
                return jnp.concatenate([val[..., :jb], val[..., jb:]], axis=1)

            def add(ref, val):
                ref[...] += val[..., :jb] + val[..., jb:]

            twice = lambda ref: lanes(ref[...], 2 * jb)
            o8 = wide(o_s)
            centered = o8 - jnp.mean(o8, axis=0, keepdims=True)
            inv_std = lax.rsqrt(jnp.mean(centered * centered, axis=0, keepdims=True) + LN_EPS)
            o_hat = centered * inv_std
            o_norm = (o_hat * twice(osc_ref) + twice(ooff_ref)).astype(BF16).reshape(chans * SUB, 2 * jb)
            upd = (nn_dot(wo_ref[...], o_norm).reshape(cz, SUB, 2 * jb) + twice(bout_ref)).astype(BF16).astype(F32)
            sig = jnp.tanh(wide(lg_v) * 0.5) * 0.5 + 0.5
            prod = sig * wide(dyt_v)
            d_upd = prod.astype(BF16)
            dgl = prod * upd * (1.0 - sig)
            add(dbg_ref, dgl)
            dgl_v[:, pair, :] = tall(dgl).astype(BF16)
            add(dbo_ref, d_upd.astype(F32))
            d_upd2 = d_upd.reshape(cz * SUB, 2 * jb)
            gram_s[...] += nt_dot(o_norm, d_upd2)
            d_on = nn_dot(wot_ref[...], d_upd2).astype(BF16).astype(F32).reshape(chans, SUB, 2 * jb)
            add(dsc_ref, d_on * o_hat)
            add(dof_ref, d_on)
            g_hat = d_on * twice(osc_ref)
            m1 = jnp.mean(g_hat, axis=0, keepdims=True)
            m2 = jnp.mean(g_hat * o_hat, axis=0, keepdims=True)
            do_v[:, pair, :] = tall(inv_std * (g_hat - m1 - o_hat * m2)).astype(BF16)
            return carry
        lax.fori_loop(0, rows // (2 * SUB), chain_body, 0)
        put_do = pltpu.make_async_copy(do_v, do_out.at[r], loc_sem.at[0])
        put_gl = pltpu.make_async_copy(dgl_v, dgl_ref.at[:, :, col], loc_sem.at[1])
        put_do.start()
        put_gl.start()
        put_do.wait()
        put_gl.wait()
        for c in ship[r]:
            if c is not None:
                c.start()

    project_rows(z_own, m_own, n_grp, lambda g: 0, lambda g: (OWN, g))
    for q in range(n_grp):
        swap(OWN, q)
    pltpu.emit_pipeline(lg_body, grid=(n_grp,), in_specs=[row3, row3], out_specs=[chan3(cz), chan3(cz)])(z_own.at[0], dy_ref, lg_ref, dyt_ref)
    swapped_b(OWN)
    chain(OWN)
    for c in masks:
        c.wait_recv()

    def sides(t, carry):
        z_r(t).wait_recv()
        z_l(n_grp - 1 - t).wait_recv()

        @pl.when(t < n_grp // 2)
        def _():
            fwd_r(t).start()
            fwd_l(n_grp - 1 - t).start()
        project_rows(z_far, m_far, 2, lambda g: g, lambda g: (g + LEFT, jnp.where(g == 0, t, n_grp - 1 - t)))
        swap(LEFT, t)
        swap(RIGHT, n_grp - 1 - t)
        return carry
    lax.fori_loop(0, n_grp, sides, 0)
    swapped_b(LEFT)
    chain(LEFT)
    swapped_b(RIGHT)
    chain(RIGHT)

    def opposite(t, carry):
        fwd_r(t).wait_recv()
        fwd_l(n_grp - 1 - t).wait_recv()
        project_rows(z_far, m_far, 2, lambda g: 2, lambda g: (OPP, jnp.where(g == 0, t, n_grp - 1 - t)))
        swap(OPP, t)
        swap(OPP, n_grp - 1 - t)
        return carry
    lax.fori_loop(0, n_grp // 2, opposite, 0)
    swapped_b(OPP)
    chain(OPP)

    gram = gram_s[...]
    n = gram.shape[0]
    diag = lax.broadcasted_iota(jnp.int32, (n, n), 0) % SUB == lax.broadcasted_iota(jnp.int32, (n, n), 1) % SUB
    gram_ref[...] = jnp.sum(jnp.where(diag, gram, 0.0).reshape(chans, SUB, n), axis=1)

    pc = 4
    n_a = chans // pc

    def da_body(do_b, b_b, da_b):
        for c in range(pc):
            lhs = jnp.concatenate([do_b[r, c] for r in range(4)], axis=1)
            rhs = jnp.concatenate([b_b[r, c] for r in range(4)], axis=0)
            da_b[c] = nn_dot(lhs, rhs).astype(BF16)

    pltpu.emit_pipeline(
        da_body, grid=(n_a,),
        in_specs=[blk((4, pc, rows, jb), lambda s: (0, s, 0, 0)), blk((4, pc, jb, cols), lambda s: (0, s, 0, 0))],
        out_specs=[blk((pc, rows, cols), lambda s: (s, 0, 0))])(do_out, b_pair, da_ref)

    for r in range(4):
        lax.fori_loop(0, n_grp, lambda q, carry, r=r: (swap_a(r, q).wait_recv(), carry)[1], 0)
        for c in ship[r]:
            if c is not None:
                c.wait_recv()

    def db_body(own_b, do0_b, do1_b, am_b, as_b, keep_b, give_b):
        for c in range(pc):
            lhs, rhs = [], []
            for r in range(4):
                lhs += [own_b[0, c] if r == OWN else do0_b[r - 1, c], do1_b[r, 0, c]]
                rhs += [am_b[r, c], as_b[r, c]]
            pair = tn_dot(jnp.concatenate(lhs, axis=0), jnp.concatenate(rhs, axis=0)).astype(BF16)
            keep_b[c] = jnp.where(low, pair[:rows], pair[rows:])
            give_b[c] = jnp.where(low, pair[rows:], pair[:rows])

    for q in (0, 1):
        steps = half // pc // 2
        at = lambda s: s + q * steps
        c3 = blk((pc, rows, cols), lambda s: (at(s), 0, 0))
        pltpu.emit_pipeline(
            db_body, grid=(steps,),
            in_specs=[blk((1, pc, rows, jb), lambda s: (0, at(s), 0, 0)), blk((3, pc, rows, jb), lambda s: (0, at(s), 0, 0)),
                      blk((4, 1, pc, rows, jb), lambda s: (0, 0, at(s), 0, 0)),
                      c4_at(pc, rows, cols, at), c4_at(pc, rows, cols, at)],
            out_specs=[c3, c3])(do_out, do_in.at[pl.ds(1, 3), 0], do_in.at[:, pl.ds(1, 1)], a_all, a_sib, keep_ref, give_ref)
        swap_d[q].start()
    for c in swap_d:
        c.wait_recv()
    for c in masks + swap_d + [c for pair in ship for c in pair if c is not None]:
        c.wait_send()

    def sent(q, carry):
        z_r(q).wait_send()
        z_l(q).wait_send()
        for r in range(4):
            for c in swap_b(r, q) + [swap_a(r, q)]:
                c.wait_send()

        @pl.when(q < n_grp // 2)
        def _():
            fwd_r(q).wait_send()

        @pl.when(q >= n_grp // 2)
        def _():
            fwd_l(q).wait_send()
        return carry
    lax.fori_loop(0, n_grp, sent, 0)


def c4_at(pc, rows, cols, at):
    return pl.BlockSpec((4, pc, rows, cols), lambda s: (0, at(s), 0, 0))


def input_kernel(z_ref, dy_ref, mask_ref, da_ref, db0_ref, db1_ref, dgl_ref, wk_ref, bias_ref, wg_ref, sc_ref, off_ref,
                 dz_ref, gram_ref, dbias_ref, dsc_ref, dof_ref, dp_s):
    chans = da_ref.shape[0]
    chan_z, cols = z_ref.shape[1:]

    @pl.when(pl.program_id(0) == 0)
    def _():
        for ref in (gram_ref, dbias_ref, dsc_ref, dof_ref):
            ref[...] = jnp.zeros_like(ref)

    def fold(val):
        acc = val[..., :128]
        for lane in range(128, cols, 128):
            acc = acc + val[..., lane:lane + 128]
        return acc

    n_p = chans * SUB
    grads = (da_ref[...].astype(F32), jnp.concatenate([db0_ref[...], db1_ref[...]], axis=0).astype(F32))
    for half in range(2):
        rows = slice(half * SUB, (half + 1) * SUB)
        z_hat, inv_std, zn = row_norm(z_ref[rows].astype(F32), sc_ref[...], off_ref[...])
        zn2 = zn.reshape(SUB * chan_z, cols)
        mask_f = mask_ref[rows].astype(F32)[None]
        for side, grad_all in enumerate(grads):
            prod = nn_dot(wk_ref[side * 2 * n_p:(side + 1) * 2 * n_p], zn2)
            val = prod[:n_p].reshape(chans, SUB, cols) + lanes(bias_ref[side * 2 * chans:side * 2 * chans + chans], cols)
            gate = prod[n_p:].reshape(chans, SUB, cols) + lanes(bias_ref[side * 2 * chans + chans:(side + 1) * 2 * chans], cols)
            sig = jnp.tanh(gate) * 0.5 + 0.5
            grad = grad_all[:, rows] * mask_f
            d_val = grad * sig
            d_gate = d_val * val * (1.0 - sig)
            dbias_ref[2 * side * chans:(2 * side + 1) * chans] += fold(d_val)
            dbias_ref[(2 * side + 1) * chans:(2 * side + 2) * chans] += fold(d_gate)
            dp_s[2 * side * n_p:(2 * side + 1) * n_p] = d_val.astype(BF16).reshape(n_p, cols)
            dp_s[(2 * side + 1) * n_p:(2 * side + 2) * n_p] = d_gate.astype(BF16).reshape(n_p, cols)
        dp_s[4 * n_p:] = dgl_ref[...].astype(F32)[:, rows].astype(BF16).reshape(n_p, cols)
        d_zn = nn_dot(wg_ref[...], dp_s[...]).astype(BF16).astype(F32).reshape(SUB, chan_z, cols)
        gram = nt_dot(zn2, dp_s[...]).reshape(SUB, chan_z, dp_s.shape[0])
        lane_row = lax.broadcasted_iota(jnp.int32, (chan_z, dp_s.shape[0]), 1) % SUB
        acc = gram_ref[...]
        for i in range(SUB):
            acc = acc + jnp.where(lane_row == i, gram[i], 0.0)
        gram_ref[...] = acc
        dsc_ref[...] += jnp.sum(d_zn * z_hat, axis=0)
        dof_ref[...] += jnp.sum(d_zn, axis=0)
        g_hat = d_zn * sc_ref[...][None]
        m1 = jnp.mean(g_hat, axis=1, keepdims=True)
        m2 = jnp.mean(g_hat * z_hat, axis=1, keepdims=True)
        d_z = dy_ref[rows].astype(F32) + inv_std * (g_hat - m1 - z_hat * m2)
        dz_ref[rows] = d_z.astype(BF16)


def whole(arr):
    nd = arr.ndim
    return pl.BlockSpec(arr.shape, lambda *_: (0,) * nd, pipeline_mode=pl.Buffered(1))


def call(kernel, name, us, *args, **kw):
    cost = pl.CostEstimate(flops=int(us * COST), bytes_accessed=2**20, transcendentals=0)
    return pl.pallas_call(kernel, name=name, cost_estimate=cost, compiler_params=pltpu.CompilerParams(vmem_limit_bytes=VMEM_LIMIT), **kw)(*args)


def local_grads(n_dap, z_loc, mask_loc, dy_loc, ln_in_scale, ln_in_offset, w_in, b_in, ln_out_scale, ln_out_offset, w_out, b_out, w_gate, b_gate):
    rows, cols, cz = z_loc.shape
    ch = w_in.shape[1] // 4
    half = ch // 2
    jb = 2 * rows
    grp = 2 * SUB
    n_grp = rows // grp
    sds = jax.ShapeDtypeStruct
    me = lax.axis_index('dap')
    core = me % 2
    z_t = jnp.transpose(z_loc, (0, 2, 1))
    dy_t = jnp.transpose(dy_loc, (0, 2, 1))

    def order(arr):
        return jnp.where(core == 0, arr, jnp.roll(arr, half, axis=0))

    n_e = 5 * ch
    b16 = lambda *shape: sds(shape, BF16)
    vecs = jnp.concatenate([ln_in_scale, ln_in_offset, ln_out_scale, ln_out_offset, b_out, b_gate, b_in]).reshape(-1, cz)
    row3 = lambda nd: pl.BlockSpec((grp, nd, cols), lambda g: (g, 0, 0))
    chan_rows = lambda n: pl.BlockSpec((n, grp, cols), lambda g: (0, g, 0))
    mask_spec = pl.BlockSpec((grp, cols), lambda g: (g, 0))
    f32 = lambda *shape: sds(shape, F32)
    any_spec = pl.BlockSpec(memory_space=pl.ANY)
    vmem = pl.BlockSpec(memory_space=pltpu.VMEM)
    n_copy = 3 + 3 * n_grp + 8 * n_grp + 4 * n_grp + 10
    acc = f32(ch, SUB, 128)
    blocks = pltpu.VMEM((ch * SUB, cz * SUB), BF16)
    spread = pltpu.VMEM((ch, SUB, 128), F32)
    outs = pl.pallas_call(
        functools.partial(front_kernel, n_dap), name='front',
        out_shape=(b16(ch, rows, cols), b16(half, rows, cols), b16(half, rows, cols), b16(cz, rows, cols), f32(ch, cz * SUB), acc, acc, acc, acc,
                   b16(n_e * SUB, SUB * cz), b16(SUB * cz, n_e * SUB), f32(n_e, SUB, 128), f32(cz, cols), f32(cz, cols),
                   b16(half, rows, cols), b16(3, rows, cz, cols), sds((3, rows, cols), jnp.int32), b16(4, ch, rows, cols), b16(4, ch, jb, cols),
                   b16(4, half, rows, cols), f32(cz, rows, cols), b16(cz, rows, cols), b16(4, ch, rows, jb), b16(4, 2, half, rows, jb)),
        in_specs=[any_spec] * 3 + [vmem] * 4,
        out_specs=(any_spec,) * 4 + (vmem,) * 10 + (any_spec,) * 10,
        scratch_shapes=[blocks, blocks, blocks, spread, spread, spread,
                        pltpu.VMEM((ch, rows, jb), F32), pltpu.VMEM((ch * SUB, cz * SUB), F32), pltpu.VMEM((cz, rows, jb), F32),
                        pltpu.VMEM((cz, rows, jb), BF16), pltpu.VMEM((ch, rows, jb), BF16), pltpu.VMEM((cz, rows, jb), BF16),
                        pltpu.SemaphoreType.DMA((n_copy,)), pltpu.SemaphoreType.DMA((n_copy,)), pltpu.SemaphoreType.DMA((2,))],
        cost_estimate=pl.CostEstimate(flops=10**11, bytes_accessed=2**20, transcendentals=0),
        compiler_params=pltpu.CompilerParams(vmem_limit_bytes=VMEM_LIMIT, collective_id=0, has_side_effects=True),
    )(z_t[None], dy_t, mask_loc[None], w_in, w_out, w_gate, vecs)
    da, keep, got, dgl, gram_o, dbg, dbo, dsc_o, dof_o, wk, wg, bias, sc_in, off_in = outs[:14]

    args = (z_t, dy_t, mask_loc, da, keep, got, dgl, wk, bias, wg, sc_in, off_in)
    const = lambda *shape: pl.BlockSpec(shape, lambda g: (0,) * len(shape))
    dz_t, gram_i, dbias, dsc_i, dof_i = call(
        input_kernel, 'input_side', 42, *args, grid=(n_grp,),
        out_shape=(b16(rows, cz, cols), sds((cz, n_e * SUB), F32), sds((4 * ch, SUB, 128), F32), sds((cz, cols), F32), sds((cz, cols), F32)),
        in_specs=[row3(cz), row3(cz), mask_spec, chan_rows(ch), chan_rows(half), chan_rows(half), chan_rows(cz)] + [whole(x) for x in args[7:]],
        out_specs=(row3(cz), const(cz, n_e * SUB), const(4 * ch, SUB, 128), const(cz, cols), const(cz, cols)),
        scratch_shapes=[pltpu.VMEM((n_e * SUB, cols), BF16)])

    d_w = jnp.transpose(gram_i.reshape(cz, n_e, SUB).sum(-1))
    d_wout = gram_o.reshape(ch, cz, SUB).sum(-1)
    tail = lambda acc: acc.sum((-2, -1))
    dbias = tail(dbias)
    by_name = lambda arr: jnp.concatenate([order(arr[i * ch:(i + 1) * ch]) for i in (0, 2, 1, 3)])
    partial = (dsc_i.sum(-1), dof_i.sum(-1), by_name(d_w), by_name(dbias), order(tail(dsc_o)), order(tail(dof_o)), order(d_wout), tail(dbo), d_w[4 * ch:], tail(dbg))
    summed = [piece.astype(BF16) for piece in lax.psum(partial, 'dap')]
    summed[2] = summed[2].T
    summed[8] = summed[8].T
    return (jnp.transpose(dz_t, (0, 2, 1)),) + tuple(summed)


def solution(mesh):
    pair_spec = P(('batch', 'dap'), None, None)
    mask_spec = P(('batch', 'dap'), None)
    vec_rep = P(None)
    mat_rep = P(None, None)
    vec_part = P('batch')
    mat_part = P('batch', None)
    in_specs = (pair_spec, mask_spec, pair_spec, vec_rep, vec_rep, mat_rep, vec_rep, vec_rep, vec_rep, mat_rep, vec_rep, mat_rep, vec_rep)
    out_specs = (pair_spec, vec_part, vec_part, mat_part, vec_part, vec_part, vec_part, mat_part, vec_part, mat_part, vec_part)
    body = functools.partial(local_grads, mesh.shape['dap'])
    return jax.shard_map(body, mesh=mesh, in_specs=in_specs, out_specs=out_specs, check_vma=False)
```

```python
import functools
import jax
import jax.numpy as jnp
from jax import lax
from jax.experimental import pallas as pl
from jax.experimental.pallas import tpu as pltpu
from jax.sharding import PartitionSpec as P

LN_EPS = 1e-5
F32 = jnp.float32
BF16 = jnp.bfloat16
SUB = 8
VMEM_LIMIT = 63 * 1024 * 1024
COST = 5e8
ZERO, ONE, TWO = range(3)
LANES = 128


def nn_dot(lhs, rhs):
    return lax.dot_general(lhs, rhs, (((ONE,), (ZERO,)), ((), ())), preferred_element_type=F32)


def nt_dot(lhs, rhs):
    return lax.dot_general(lhs, rhs, (((ONE,), (ONE,)), ((), ())), preferred_element_type=F32)


def tn_dot(lhs, rhs):
    return lax.dot_general(lhs, rhs, (((ZERO,), (ZERO,)), ((), ())), preferred_element_type=F32)


def row_norm(z8, scale, offset):
    mean_val = jnp.mean(z8, axis=ONE, keepdims=True)
    centered = z8 - mean_val
    inv_std = lax.rsqrt(jnp.mean(centered * centered, axis=ONE, keepdims=True) + LN_EPS)
    z_hat = centered * inv_std
    return z_hat, inv_std, (z_hat * scale[None] + offset[None]).astype(BF16)


def lanes(bias, width):
    return jnp.concatenate([bias] * (width // bias.shape[-ONE]), axis=-ONE)


def gated(prod, bias_ref, start, chans, mask_half):
    cols = prod.shape[-ONE]
    val = prod[:chans * SUB].reshape(chans, SUB, cols) + lanes(bias_ref[start:start + chans], cols)
    gate = prod[chans * SUB:].reshape(chans, SUB, cols) + lanes(bias_ref[start + chans:start + TWO * chans], cols)
    return (jnp.tanh(gate) + 1.0) * (val * mask_half[None])


def build_weights(core, w_in, w_out, w_gate, vecs, wk_ref, wg_ref, bias_ref, sc_ref, off_ref, perm_s, wok_s, wotk_s, bo_s, osc_s, ooff_s):
    cz = w_in.shape[ZERO]
    ch = w_in.shape[ONE] // 4
    big = ch * SUB

    def iota(shape, dim):
        return lax.broadcasted_iota(jnp.int32, shape, dim)

    def one(cond):
        return jnp.where(cond, 1.0, 0.0).astype(BF16)

    turn = core * (ch // TWO)
    rep = iota((big, ch), ZERO) // SUB == iota((big, ch), ONE)
    rep_c = lax.rem(iota((big, ch), ZERO) // SUB + turn, ch) == iota((big, ch), ONE)
    rep_t = iota((ch, big), ONE) // SUB == iota((ch, big), ZERO)
    rep_ct = lax.rem(iota((ch, big), ONE) // SUB + turn, ch) == iota((ch, big), ZERO)
    tile = one(iota((cz, SUB * cz), ONE) % cz == iota((cz, SUB * cz), ZERO))
    tile_t = one(iota((SUB * cz, cz), ZERO) % cz == iota((SUB * cz, cz), ONE))
    keep = iota((big, SUB * cz), ZERO) % SUB == iota((big, SUB * cz), ONE) // cz
    keep_t = iota((SUB * cz, big), ONE) % SUB == iota((SUB * cz, big), ZERO) // cz
    same = iota((big, big), ZERO) % SUB == iota((big, big), ONE) % SUB

    def spread(wide):
        return jnp.where(keep, nn_dot(wide, tile), 0.0).astype(BF16)

    def column(sel, row, width):
        picked = jnp.where(sel, jnp.broadcast_to(row.astype(F32), sel.shape), 0.0).astype(BF16)
        return nn_dot(picked, jnp.ones((sel.shape[ONE], width), BF16))

    def eights(sel, row):
        return column(sel, row, LANES).reshape(ch, SUB, LANES)

    for dst, src, scale in ((ZERO, ZERO, 1.0), (ONE, TWO, 0.5), (TWO, ONE, 1.0), (3, 3, 0.5), (4, None, 1.0)):
        w_part = w_gate[...] if src is None else w_in[:, src * ch:(src + ONE) * ch]
        sel, sel_t = (rep, rep_t) if src is None else (rep_c, rep_ct)
        at = slice(dst * big, (dst + ONE) * big)
        wide = (nt_dot(one(sel), w_part) * scale).astype(BF16)
        wk_ref[at] = spread(wide)
        wg_ref[:, at] = jnp.where(keep_t, nn_dot(tile_t, nn_dot(w_part, one(sel_t)).astype(BF16)), 0.0).astype(BF16)
        vec = 5 if src is None else 6 + src
        bias_ref[dst * ch:(dst + ONE) * ch] = eights(sel, vecs[vec]) * scale
    eye = iota((cz, cz), ZERO) == iota((cz, cz), ONE)
    perm_s[...] = spread(one(rep))
    wok_s[...] = jnp.where(same, nn_dot(nt_dot(one(rep), w_out[...]).astype(BF16), one(rep_ct)), 0.0).astype(BF16)
    wotk_s[...] = jnp.where(same, nn_dot(nn_dot(one(rep_c), w_out[...]).astype(BF16), one(rep_t)), 0.0).astype(BF16)
    sc_ref[...] = column(eye, vecs[ZERO], sc_ref.shape[ONE])
    off_ref[...] = column(eye, vecs[ONE], off_ref.shape[ONE])
    osc_s[...] = eights(rep_c, vecs[TWO])
    ooff_s[...] = eights(rep_c, vecs[3])
    bo_s[...] = eights(rep, vecs[4])


def gate_parts(prod, bias_ref, start, chans):
    cols = prod.shape[-ONE]
    val = prod[:chans * SUB].reshape(chans, SUB, cols) + lanes(bias_ref[start:start + chans], cols)
    gate = prod[chans * SUB:].reshape(chans, SUB, cols) + lanes(bias_ref[start + chans:start + TWO * chans], cols)
    return val, jnp.tanh(gate) * 0.5 + 0.5


def project(z8, mask_half, wk_ref, bias_ref, sc_ref, off_ref, chans):
    cols = z8.shape[-ONE]
    _, _, zn = row_norm(z8.astype(F32), sc_ref[...], off_ref[...])
    zn2 = zn.reshape(SUB * zn.shape[ONE], cols)
    n_p = TWO * chans * SUB
    act_a = gated(nn_dot(wk_ref[:n_p], zn2), bias_ref, ZERO, chans, mask_half)
    act_b = gated(nn_dot(wk_ref[n_p:TWO * n_p], zn2), bias_ref, TWO * chans, chans, mask_half)
    return act_a, act_b, zn2


MESH = pl.DeviceIdType.MESH
OWN, LEFT, RIGHT, OPP = range(4)
HOPS = (ZERO, -ONE, ONE, TWO)


def blk(shape, index_map):
    return pl.BlockSpec(shape, index_map)


def front_kernel(n_dap, z_own, dy_ref, m_own, w_in, w_out, w_gate, v_is, v_io, v_os, v_oo, v_bo, v_bg, v_bi,
                 da_ref, keep_ref, got_ref, dgl_ref, gram_ref, dbg_ref, dbo_ref, dsc_ref, dof_ref, wg_ref, sc_ref, off_ref,
                 sv_ref, give_ref, z_far, m_far, a_all, b_pair, a_sib, lg_ref, dyt_ref, do_out, do_in,
                 wk_ref, bias_ref, perm_ref, wo_ref, wot_ref, bout_ref, osc_ref, ooff_ref,
                 o_s, gram_s, lg_v, dyt_v, do_v, dgl_v, send_sem, recv_sem, loc_sem):
    n_chip = n_dap // TWO
    _, rows, cz, cols = z_own.shape
    z_ref, mask_ref = z_own.at[ZERO], m_own.at[ZERO]
    chans = a_all.shape[ONE]
    half = chans // TWO
    hr = rows // TWO
    jb = TWO * rows
    grp = TWO * SUB
    me = lax.axis_index('dap')
    core, chip = lax.rem(me, TWO), me // TWO
    low = core == ZERO

    def peer(hop, flip):
        to = lax.rem(chip + (hop + n_chip), n_chip) * TWO
        return {'dap': to + (ONE - core if flip else core)}

    def copy(k, src, dst, hop, flip):
        return pltpu.make_async_remote_copy(src_ref=src, dst_ref=dst, send_sem=send_sem.at[k], recv_sem=recv_sem.at[k],
                                            device_id=peer(hop, flip), device_id_type=MESH)

    barrier = pltpu.get_barrier_semaphore()
    for hop in HOPS:
        for flip in (ZERO, ONE):
            if hop or flip:
                pl.semaphore_signal(barrier, inc=ONE, device_id=peer(hop, flip), device_id_type=MESH)
    pl.semaphore_wait(barrier, n_dap - ONE)

    n_grp = rows // grp
    masks = [copy(i, mask_ref, m_far.at[i], hop, ZERO) for i, hop in enumerate((ONE, -ONE, TWO))]
    quarter = lambda q: pl.ds(pl.multiple_of(q * grp, grp), grp)
    z_r = lambda q: copy(3 + q, z_ref.at[quarter(q)], z_far.at[ZERO, quarter(q)], ONE, ZERO)
    z_l = lambda q: copy(3 + n_grp + q, z_ref.at[quarter(q)], z_far.at[ONE, quarter(q)], -ONE, ZERO)
    fwd_r = lambda q: copy(3 + TWO * n_grp + q, z_far.at[ZERO, quarter(q)], z_far.at[TWO, quarter(q)], ONE, ZERO)
    fwd_l = lambda q: copy(3 + TWO * n_grp + q, z_far.at[ONE, quarter(q)], z_far.at[TWO, quarter(q)], -ONE, ZERO)
    base_b = 3 + 3 * n_grp
    my_rows = pl.multiple_of(core * rows, rows)

    def swap_b(r, q):
        at = pl.ds(pl.multiple_of(my_rows + q * grp, grp), grp)
        return [copy(base_b + (r * n_grp + q) * TWO + h, b_pair.at[r, pl.ds(h * half, half), at], b_pair.at[r, pl.ds((ONE - h) * half, half), at], ZERO, ONE) for h in (ZERO, ONE)]

    base_a = base_b + 8 * n_grp
    swap_a = lambda r, q: copy(base_a + r * n_grp + q, a_all.at[r, pl.ds(half, half), quarter(q)], a_sib.at[r, :, quarter(q)], ZERO, ONE)
    base_s = base_a + 4 * n_grp
    back = (OWN, RIGHT, LEFT, OPP)
    ship = [[None if (r == OWN and side == ZERO) else
             copy(base_s + TWO * r + side, do_out.at[r, pl.ds(side * half, half)], do_in.at[back[r], side], HOPS[r], side) for side in (ZERO, ONE)] for r in range(4)]
    swap_d = [copy(base_s + 8 + q, give_ref.at[pl.ds(q * (half // TWO), half // TWO)], got_ref.at[pl.ds(q * (half // TWO), half // TWO)], ZERO, ONE) for q in (ZERO, ONE)]

    for c in masks:
        c.start()
    for q in range(n_grp):
        z_r(q).start()
        z_l(n_grp - ONE - q).start()
    b_all = v_bi[...]
    vecs = [ref[...] for ref in (v_is, v_io, v_os, v_oo, v_bo, v_bg)] + [b_all[:, i * chans:(i + ONE) * chans] for i in range(4)]
    build_weights(core, w_in, w_out, w_gate, vecs, wk_ref, wg_ref, bias_ref, sc_ref, off_ref, perm_ref, wo_ref, wot_ref, bout_ref, osc_ref, ooff_ref)

    row3 = blk((grp, cz, cols), lambda g: (g, ZERO, ZERO))
    row2 = blk((grp, cols), lambda g: (g, ZERO))
    chan3 = lambda n: blk((n, grp, cols), lambda g: (ZERO, g, ZERO))

    def ab_body(z_b, m_b, a_b, b_b):
        a_parts, b_parts = [], []
        for h in range(TWO):
            rws = slice(h * SUB, (h + ONE) * SUB)
            act_a, act_b, _ = project(z_b[ZERO, rws], m_b[ZERO, rws].astype(F32) * 0.5, wk_ref, bias_ref, sc_ref, off_ref, chans)
            a_parts.append(act_a)
            b_parts.append(act_b)
        a_b[ZERO] = jnp.concatenate(a_parts, axis=ONE).astype(BF16)
        b_b[ZERO] = jnp.concatenate(b_parts, axis=ONE).astype(BF16)

    def own_body(z_b, m_b, a_b, b_b, sv_b):
        acts = ([], [])
        for h in range(TWO):
            rws = slice(h * SUB, (h + ONE) * SUB)
            _, _, zn = row_norm(z_b[ZERO, rws].astype(F32), sc_ref[...], off_ref[...])
            zn2 = zn.reshape(SUB * cz, cols)
            mask = m_b[ZERO, rws].astype(F32)[None]
            n_p = TWO * chans * SUB
            for side in (ZERO, ONE):
                val, sig = gate_parts(nn_dot(wk_ref[side * n_p:(side + ONE) * n_p], zn2), bias_ref, TWO * side * chans, chans)
                sv_b[TWO * side, :, rws] = val
                sv_b[TWO * side + ONE, :, rws] = sig
                acts[side].append(mask * sig * val)
        a_b[ZERO] = jnp.concatenate(acts[ZERO], axis=ONE).astype(BF16)
        b_b[ZERO] = jnp.concatenate(acts[ONE], axis=ONE).astype(BF16)

    def project_rows(z_src, m_src, n, slot, place):
        pltpu.emit_pipeline(
            ab_body, grid=(n,),
            in_specs=[blk((ONE, grp, cz, cols), lambda g: (slot(g), place(g)[ONE], ZERO, ZERO)), blk((ONE, grp, cols), lambda g: (slot(g), place(g)[ONE], ZERO))],
            out_specs=[blk((ONE, chans, grp, cols), lambda g: (place(g)[ZERO], ZERO, place(g)[ONE], ZERO)),
                       blk((ONE, chans, grp, cols), lambda g: (place(g)[ZERO], ZERO, core * n_grp + place(g)[ONE], ZERO))])(z_src, m_src, a_all, b_pair)

    def swap(r, q):
        for c in swap_b(r, q):
            c.start()
        swap_a(r, q).start()

    def swapped_b(r):
        def body(q, carry):
            for c in swap_b(r, q):
                c.wait_recv()
            return carry
        lax.fori_loop(ZERO, n_grp, body, ZERO)

    def lg_body(z_b, dy_b, lg_b, dyt_b):
        dy_parts = []
        for h in range(TWO):
            rws = slice(h * SUB, (h + ONE) * SUB)
            _, _, zn = row_norm(z_b[rws].astype(F32), sc_ref[...], off_ref[...])
            zn2 = zn.reshape(SUB * cz, cols)
            lg_b[:, rws, :] = nn_dot(wk_ref[4 * chans * SUB:], zn2).reshape(cz, SUB, cols) + lanes(bias_ref[4 * chans:], cols)
            dy_parts.append(nn_dot(perm_ref[...], dy_b[rws].reshape(SUB * cz, cols)).reshape(cz, SUB, cols))
        dyt_b[...] = jnp.concatenate(dy_parts, axis=ONE).astype(BF16)

    for ref in (dbg_ref, dbo_ref, dsc_ref, dof_ref, gram_s):
        ref[...] = jnp.zeros_like(ref)

    per = chans // 8

    def o_body(a_b, b_b):
        base = pl.program_id(ZERO) * per
        for c in range(per):
            o_s[base + c] = nt_dot(a_b[c], b_b[c])

    def chain(r):
        where = lax.rem(chip + (HOPS[r] + n_chip), n_chip)
        col = pl.ds(pl.multiple_of(where * jb, jb), jb)
        get_lg = pltpu.make_async_copy(lg_ref.at[:, :, col], lg_v, loc_sem.at[ZERO])
        get_dy = pltpu.make_async_copy(dyt_ref.at[:, :, col], dyt_v, loc_sem.at[ONE])
        get_lg.start()
        get_dy.start()
        pltpu.emit_pipeline(o_body, grid=(8,), in_specs=[blk((per, rows, cols), lambda s: (s, ZERO, ZERO)), blk((per, jb, cols), lambda s: (s, ZERO, ZERO))])(
            a_all.at[OWN], b_pair.at[r])
        get_lg.wait()
        get_dy.wait()

        def chain_body(g, carry):
            pair = pl.ds(pl.multiple_of(g * TWO * SUB, TWO * SUB), TWO * SUB)

            def wide(ref):
                val = ref[:, pair, :].astype(F32)
                return jnp.concatenate([val[:, :SUB], val[:, SUB:]], axis=TWO)

            def tall(val):
                return jnp.concatenate([val[..., :jb], val[..., jb:]], axis=ONE)

            def add(ref, val):
                ref[...] += val[..., :jb] + val[..., jb:]

            twice = lambda ref: lanes(ref[...], TWO * jb)
            o8 = wide(o_s)
            centered = o8 - jnp.mean(o8, axis=ZERO, keepdims=True)
            inv_std = lax.rsqrt(jnp.mean(centered * centered, axis=ZERO, keepdims=True) + LN_EPS)
            o_hat = centered * inv_std
            o_norm = (o_hat * twice(osc_ref) + twice(ooff_ref)).astype(BF16).reshape(chans * SUB, TWO * jb)
            upd = (nn_dot(wo_ref[...], o_norm).reshape(cz, SUB, TWO * jb) + twice(bout_ref)).astype(BF16).astype(F32)
            sig = jnp.tanh(wide(lg_v) * 0.5) * 0.5 + 0.5
            prod = sig * wide(dyt_v)
            d_upd = prod.astype(BF16)
            dgl = prod * upd * (1.0 - sig)
            add(dbg_ref, dgl)
            dgl_v[:, pair, :] = tall(dgl).astype(BF16)
            add(dbo_ref, d_upd.astype(F32))
            d_upd2 = d_upd.reshape(cz * SUB, TWO * jb)
            gram_s[...] += nt_dot(o_norm, d_upd2)
            d_on = nn_dot(wot_ref[...], d_upd2).astype(BF16).astype(F32).reshape(chans, SUB, TWO * jb)
            add(dsc_ref, d_on * o_hat)
            add(dof_ref, d_on)
            g_hat = d_on * twice(osc_ref)
            m1 = jnp.mean(g_hat, axis=ZERO, keepdims=True)
            m2 = jnp.mean(g_hat * o_hat, axis=ZERO, keepdims=True)
            do_v[:, pair, :] = tall(inv_std * (g_hat - m1 - o_hat * m2)).astype(BF16)
            return carry
        lax.fori_loop(ZERO, rows // (TWO * SUB), chain_body, ZERO)
        put_do = pltpu.make_async_copy(do_v, do_out.at[r], loc_sem.at[ZERO])
        put_gl = pltpu.make_async_copy(dgl_v, dgl_ref.at[:, :, col], loc_sem.at[ONE])
        put_do.start()
        put_gl.start()
        put_do.wait()
        put_gl.wait()
        for c in ship[r]:
            if c is not None:
                c.start()

    pltpu.emit_pipeline(
        own_body, grid=(n_grp,),
        in_specs=[blk((ONE, grp, cz, cols), lambda g: (ZERO, g, ZERO, ZERO)), blk((ONE, grp, cols), lambda g: (ZERO, g, ZERO))],
        out_specs=[blk((ONE, chans, grp, cols), lambda g: (OWN, ZERO, g, ZERO)), blk((ONE, chans, grp, cols), lambda g: (OWN, ZERO, core * n_grp + g, ZERO)),
                   blk((4, chans, grp, cols), lambda g: (ZERO, ZERO, g, ZERO))])(z_own, m_own, a_all, b_pair, sv_ref)
    for q in range(n_grp):
        swap(OWN, q)
    pltpu.emit_pipeline(lg_body, grid=(n_grp,), in_specs=[row3, row3], out_specs=[chan3(cz), chan3(cz)])(z_own.at[ZERO], dy_ref, lg_ref, dyt_ref)
    swapped_b(OWN)
    chain(OWN)
    for c in masks:
        c.wait_recv()

    def sides(t, carry):
        z_r(t).wait_recv()
        z_l(n_grp - ONE - t).wait_recv()

        @pl.when(t < n_grp // TWO)
        def _():
            fwd_r(t).start()
            fwd_l(n_grp - ONE - t).start()
        project_rows(z_far, m_far, TWO, lambda g: g, lambda g: (g + LEFT, jnp.where(g == ZERO, t, n_grp - ONE - t)))
        swap(LEFT, t)
        swap(RIGHT, n_grp - ONE - t)
        return carry
    lax.fori_loop(ZERO, n_grp, sides, ZERO)
    swapped_b(LEFT)
    chain(LEFT)
    swapped_b(RIGHT)
    chain(RIGHT)

    def opposite(t, carry):
        fwd_r(t).wait_recv()
        fwd_l(n_grp - ONE - t).wait_recv()
        project_rows(z_far, m_far, TWO, lambda g: TWO, lambda g: (OPP, jnp.where(g == ZERO, t, n_grp - ONE - t)))
        swap(OPP, t)
        swap(OPP, n_grp - ONE - t)
        return carry
    lax.fori_loop(ZERO, n_grp // TWO, opposite, ZERO)
    swapped_b(OPP)
    chain(OPP)

    gram = gram_s[...]
    n = gram.shape[ZERO]
    diag = lax.broadcasted_iota(jnp.int32, (n, n), ZERO) % SUB == lax.broadcasted_iota(jnp.int32, (n, n), ONE) % SUB
    gram_ref[...] = jnp.sum(jnp.where(diag, gram, 0.0).reshape(chans, SUB, n), axis=ONE)

    pc = 4
    n_a = chans // pc

    def da_body(do_b, b_b, da_b):
        for c in range(pc):
            lhs = jnp.concatenate([do_b[r, c] for r in range(4)], axis=ONE)
            rhs = jnp.concatenate([b_b[r, c] for r in range(4)], axis=ZERO)
            da_b[c] = nn_dot(lhs, rhs).astype(BF16)

    pltpu.emit_pipeline(
        da_body, grid=(n_a,),
        in_specs=[blk((4, pc, rows, jb), lambda s: (ZERO, s, ZERO, ZERO)), blk((4, pc, jb, cols), lambda s: (ZERO, s, ZERO, ZERO))],
        out_specs=[blk((pc, rows, cols), lambda s: (s, ZERO, ZERO))])(do_out, b_pair, da_ref)

    for r in range(4):
        lax.fori_loop(ZERO, n_grp, lambda q, carry, r=r: (swap_a(r, q).wait_recv(), carry)[ONE], ZERO)
        for c in ship[r]:
            if c is not None:
                c.wait_recv()

    def db_body(own_b, do0_b, do1_b, am_b, as_b, keep_b, give_b):
        for c in range(pc):
            lhs, rhs = [], []
            for r in range(4):
                lhs += [own_b[ZERO, c] if r == OWN else do0_b[r - ONE, c], do1_b[r, ZERO, c]]
                rhs += [am_b[r, c], as_b[r, c]]
            pair = tn_dot(jnp.concatenate(lhs, axis=ZERO), jnp.concatenate(rhs, axis=ZERO)).astype(BF16)
            keep_b[c] = jnp.where(low, pair[:rows], pair[rows:])
            give_b[c] = jnp.where(low, pair[rows:], pair[:rows])

    for q in (ZERO, ONE):
        steps = half // pc // TWO
        at = lambda s: s + q * steps
        c3 = blk((pc, rows, cols), lambda s: (at(s), ZERO, ZERO))
        pltpu.emit_pipeline(
            db_body, grid=(steps,),
            in_specs=[blk((ONE, pc, rows, jb), lambda s: (ZERO, at(s), ZERO, ZERO)), blk((3, pc, rows, jb), lambda s: (ZERO, at(s), ZERO, ZERO)),
                      blk((4, ONE, pc, rows, jb), lambda s: (ZERO, ZERO, at(s), ZERO, ZERO)),
                      c4_at(pc, rows, cols, at), c4_at(pc, rows, cols, at)],
            out_specs=[c3, c3])(do_out, do_in.at[pl.ds(ONE, 3), ZERO], do_in.at[:, pl.ds(ONE, ONE)], a_all, a_sib, keep_ref, give_ref)
        swap_d[q].start()
    for c in swap_d:
        c.wait_recv()
    for c in masks + swap_d + [c for pair in ship for c in pair if c is not None]:
        c.wait_send()

    def sent(q, carry):
        z_r(q).wait_send()
        z_l(q).wait_send()
        for r in range(4):
            for c in swap_b(r, q) + [swap_a(r, q)]:
                c.wait_send()

        @pl.when(q < n_grp // TWO)
        def _():
            fwd_r(q).wait_send()

        @pl.when(q >= n_grp // TWO)
        def _():
            fwd_l(q).wait_send()
        return carry
    lax.fori_loop(ZERO, n_grp, sent, ZERO)


def c4_at(pc, rows, cols, at):
    return pl.BlockSpec((4, pc, rows, cols), lambda s: (ZERO, at(s), ZERO, ZERO))


def input_kernel(z_ref, dy_ref, mask_ref, da_ref, db0_ref, db1_ref, dgl_ref, sv_ref, wg_ref, sc_ref, off_ref,
                 dz_ref, gram_ref, dbias_ref, dsc_ref, dof_ref, dp_s):
    chans = da_ref.shape[ZERO]
    chan_z, cols = z_ref.shape[ONE:]

    @pl.when(pl.program_id(ZERO) == ZERO)
    def _():
        for ref in (gram_ref, dbias_ref, dsc_ref, dof_ref):
            ref[...] = jnp.zeros_like(ref)

    def fold(val):
        acc = val[..., :LANES]
        for lane in range(LANES, cols, LANES):
            acc = acc + val[..., lane:lane + LANES]
        return acc

    n_p = chans * SUB
    grads = (da_ref[...].astype(F32), jnp.concatenate([db0_ref[...], db1_ref[...]], axis=ZERO).astype(F32))
    for half in range(TWO):
        rows = slice(half * SUB, (half + ONE) * SUB)
        z_hat, inv_std, zn = row_norm(z_ref[rows].astype(F32), sc_ref[...], off_ref[...])
        zn2 = zn.reshape(SUB * chan_z, cols)
        mask_f = mask_ref[rows].astype(F32)[None]
        for side, grad_all in enumerate(grads):
            val, sig = sv_ref[TWO * side, :, rows], sv_ref[TWO * side + ONE, :, rows]
            grad = grad_all[:, rows] * mask_f
            d_val = grad * sig
            d_gate = d_val * val * (1.0 - sig)
            dbias_ref[TWO * side * chans:(TWO * side + ONE) * chans] += fold(d_val)
            dbias_ref[(TWO * side + ONE) * chans:(TWO * side + TWO) * chans] += fold(d_gate)
            dp_s[TWO * side * n_p:(TWO * side + ONE) * n_p] = d_val.astype(BF16).reshape(n_p, cols)
            dp_s[(TWO * side + ONE) * n_p:(TWO * side + TWO) * n_p] = d_gate.astype(BF16).reshape(n_p, cols)
        dp_s[4 * n_p:] = dgl_ref[...].astype(F32)[:, rows].astype(BF16).reshape(n_p, cols)
        d_zn = nn_dot(wg_ref[...], dp_s[...]).astype(BF16).astype(F32).reshape(SUB, chan_z, cols)
        gram = nt_dot(zn2, dp_s[...]).reshape(SUB, chan_z, dp_s.shape[ZERO])
        lane_row = lax.broadcasted_iota(jnp.int32, (chan_z, dp_s.shape[ZERO]), ONE) % SUB
        acc = gram_ref[...]
        for i in range(SUB):
            acc = acc + jnp.where(lane_row == i, gram[i], 0.0)
        gram_ref[...] = acc
        dsc_ref[...] += jnp.sum(d_zn * z_hat, axis=ZERO)
        dof_ref[...] += jnp.sum(d_zn, axis=ZERO)
        g_hat = d_zn * sc_ref[...][None]
        m1 = jnp.mean(g_hat, axis=ONE, keepdims=True)
        m2 = jnp.mean(g_hat * z_hat, axis=ONE, keepdims=True)
        d_z = dy_ref[rows].astype(F32) + inv_std * (g_hat - m1 - z_hat * m2)
        dz_ref[rows] = d_z.astype(BF16)


def exact_dot(lhs, rhs, dims):
    return lax.dot_general(lhs, rhs, (dims, ((), ())), precision=lax.Precision.HIGHEST, preferred_element_type=F32)


def sum_kernel(n_dap, gram_i, dbias, dsc_i, dof_i, gram_o, dsc_o, dof_o, dbo, dbg, out_ref, part_s, in_s, mine_s, send_sem, recv_sem, send2, recv2):
    me = lax.axis_index('dap')
    core = lax.rem(me, TWO)
    low = core == ZERO
    barrier = pltpu.get_barrier_semaphore()
    to = [lax.rem(me + d, n_dap) for d in range(n_dap)]
    for d in range(ONE, n_dap):
        pl.semaphore_signal(barrier, inc=ONE, device_id={'dap': to[d]}, device_id_type=MESH)
    cz = gram_i.shape[ZERO]
    ch = gram_o.shape[ZERO]
    big = ch * SUB
    turn = core * (ch // TWO)
    row = lax.broadcasted_iota(jnp.int32, (big, ch), ZERO) // SUB
    col = lax.broadcasted_iota(jnp.int32, (big, ch), ONE)
    fold = jnp.where(row == col, 1.0, 0.0)
    fold_c = jnp.where(lax.rem(row + turn, ch) == col, 1.0, 0.0)
    part_s[...] = jnp.zeros_like(part_s)
    for dst, src in ((ZERO, ZERO), (ONE, TWO), (TWO, ONE), (3, 3), (4, 4)):
        val = exact_dot(gram_i[:, dst * big:(dst + ONE) * big], fold if src == 4 else fold_c, ((ONE,), (ZERO,)))
        part_s[(src // TWO) * cz:(src // TWO + ONE) * cz, (src % TWO) * ch:(src % TWO + ONE) * ch] = val
    val = exact_dot(gram_o[...], fold, ((ONE,), (ZERO,)))
    h = ch // TWO
    val = jnp.where(low, val, jnp.concatenate([val[h:], val[:h]], axis=ZERO))
    part_s[TWO * cz:3 * cz, ch:TWO * ch] = val
    eye = lax.broadcasted_iota(jnp.int32, (ch, ch), ZERO)
    lane = lax.broadcasted_iota(jnp.int32, (ch, ch), ONE)
    order = jnp.where(lax.rem(eye + turn, ch) == lane, 1.0, 0.0)

    def line(acc, ordered):
        flat = jnp.sum(acc, axis=ONE) if len(acc.shape) == 3 else acc
        res = exact_dot(jnp.ones((SUB, flat.shape[ONE]), F32), flat, ((ONE,), (ONE,)))
        return exact_dot(res, order, ((ONE,), (ZERO,)))[:ONE] if ordered else res[:ONE]

    base = 3 * cz
    for dst, src in ((ZERO, ZERO), (ONE, TWO), (TWO, ONE), (3, 3)):
        part_s[base + src // TWO:base + src // TWO + ONE, (src % TWO) * ch:(src % TWO + ONE) * ch] = line(dbias[dst * ch:(dst + ONE) * ch], True)
    part_s[base + TWO:base + 3, :ch] = line(dsc_i[...], False)
    part_s[base + TWO:base + 3, ch:TWO * ch] = line(dof_i[...], False)
    part_s[base + 3:base + 4, :ch] = line(dsc_o[...], True)
    part_s[base + 3:base + 4, ch:TWO * ch] = line(dof_o[...], True)
    part_s[base + 4:base + 5, :ch] = line(dbo[...], False)
    part_s[base + 4:base + 5, ch:TWO * ch] = line(dbg[...], False)

    pl.semaphore_wait(barrier, n_dap - ONE)
    n = mine_s.shape[ZERO]

    def scatter(d):
        return pltpu.make_async_remote_copy(src_ref=part_s.at[pl.ds(pl.multiple_of(to[d] * n, n), n)], dst_ref=in_s.at[d - ONE],
                                            send_sem=send_sem.at[d - ONE], recv_sem=recv_sem.at[d - ONE],
                                            device_id={'dap': to[d]}, device_id_type=MESH)

    at = pl.ds(pl.multiple_of(me * n, n), n)

    def spread(d):
        return pltpu.make_async_remote_copy(src_ref=mine_s, dst_ref=out_ref.at[at], send_sem=send2.at[d - ONE], recv_sem=recv2.at[d - ONE],
                                            device_id={'dap': to[d]}, device_id_type=MESH)

    for d in range(ONE, n_dap):
        scatter(d).start()
    total = part_s[at]
    for d in range(ONE, n_dap):
        scatter(d).wait_recv()
        total = total + in_s[d - ONE]
    mine_s[...] = total
    for d in range(ONE, n_dap):
        spread(d).start()
    out_ref[at] = total
    for d in range(ONE, n_dap):
        spread(d).wait_recv()
    for d in range(ONE, n_dap):
        scatter(d).wait_send()
        spread(d).wait_send()


def round_kernel(tot_ref, sc_ref, off_ref, w_ref, b_ref, osc_ref, ooff_ref, wout_ref, bout_ref, wg_ref, bg_ref):
    cz, ch = wg_ref.shape
    tot = tot_ref[...].astype(BF16)
    base = 3 * cz
    w_ref[:, :TWO * ch] = tot[:cz]
    w_ref[:, TWO * ch:] = tot[cz:TWO * cz]
    wg_ref[...] = tot[TWO * cz:3 * cz, :ch]
    wout_ref[...] = tot[TWO * cz:3 * cz, ch:]
    vec = tot_ref[base:base + SUB]
    for ref, r, c in ((b_ref, ZERO, ZERO), (sc_ref, TWO, ZERO), (off_ref, TWO, ONE), (osc_ref, 3, ZERO), (ooff_ref, 3, ONE), (bout_ref, 4, ZERO), (bg_ref, 4, ONE)):
        if ref is b_ref:
            ref[:, :TWO * ch] = vec[ZERO:ONE].astype(BF16)
            ref[:, TWO * ch:] = vec[ONE:TWO].astype(BF16)
        else:
            ref[...] = vec[r:r + ONE, c * ch:(c + ONE) * ch].astype(BF16)


def whole(arr):
    nd = arr.ndim
    return pl.BlockSpec(arr.shape, lambda *_: (ZERO,) * nd, pipeline_mode=pl.Buffered(ONE))


def call(kernel, name, us, *args, **kw):
    cost = pl.CostEstimate(flops=int(us * COST), bytes_accessed=TWO**20, transcendentals=ZERO)
    return pl.pallas_call(kernel, name=name, cost_estimate=cost, compiler_params=pltpu.CompilerParams(vmem_limit_bytes=VMEM_LIMIT), **kw)(*args)


def local_grads(n_dap, z_loc, mask_loc, dy_loc, ln_in_scale, ln_in_offset, w_in, b_in, ln_out_scale, ln_out_offset, w_out, b_out, w_gate, b_gate):
    rows, cols, cz = z_loc.shape
    ch = w_in.shape[ONE] // 4
    half = ch // TWO
    jb = TWO * rows
    grp = TWO * SUB
    n_grp = rows // grp
    sds = jax.ShapeDtypeStruct
    z_t = jnp.transpose(z_loc, (ZERO, TWO, ONE))
    dy_t = jnp.transpose(dy_loc, (ZERO, TWO, ONE))

    n_e = 5 * ch
    b16 = lambda *shape: sds(shape, BF16)
    vecs = [v.reshape(ONE, -ONE) for v in (ln_in_scale, ln_in_offset, ln_out_scale, ln_out_offset, b_out, b_gate, b_in)]
    row3 = lambda nd: pl.BlockSpec((grp, nd, cols), lambda g: (g, ZERO, ZERO))
    chan_rows = lambda n: pl.BlockSpec((n, grp, cols), lambda g: (ZERO, g, ZERO))
    mask_spec = pl.BlockSpec((grp, cols), lambda g: (g, ZERO))
    f32 = lambda *shape: sds(shape, F32)
    any_spec = pl.BlockSpec(memory_space=pl.ANY)
    vmem = pl.BlockSpec(memory_space=pltpu.VMEM)
    n_copy = 3 + 3 * n_grp + 8 * n_grp + 4 * n_grp + 10
    acc = f32(ch, SUB, LANES)
    blocks = pltpu.VMEM((ch * SUB, cz * SUB), BF16)
    spread = pltpu.VMEM((ch, SUB, LANES), F32)
    outs = pl.pallas_call(
        functools.partial(front_kernel, n_dap), name='front',
        out_shape=(b16(ch, rows, cols), b16(half, rows, cols), b16(half, rows, cols), b16(cz, rows, cols), f32(ch, cz * SUB), acc, acc, acc, acc,
                   b16(SUB * cz, n_e * SUB), f32(cz, cols), f32(cz, cols),
                   f32(4, ch, rows, cols), b16(half, rows, cols), b16(3, rows, cz, cols), sds((3, rows, cols), jnp.int32), b16(4, ch, rows, cols), b16(4, ch, jb, cols),
                   b16(4, half, rows, cols), f32(cz, rows, cols), b16(cz, rows, cols), b16(4, ch, rows, jb), b16(4, TWO, half, rows, jb)),
        in_specs=[any_spec] * 3 + [vmem] * 10,
        out_specs=(any_spec,) * 4 + (vmem,) * 8 + (any_spec,) * 11,
        scratch_shapes=[pltpu.VMEM((n_e * SUB, SUB * cz), BF16), pltpu.VMEM((n_e, SUB, LANES), F32), blocks, blocks, blocks, spread, spread, spread,
                        pltpu.VMEM((ch, rows, jb), F32), pltpu.VMEM((ch * SUB, cz * SUB), F32), pltpu.VMEM((cz, rows, jb), F32),
                        pltpu.VMEM((cz, rows, jb), BF16), pltpu.VMEM((ch, rows, jb), BF16), pltpu.VMEM((cz, rows, jb), BF16),
                        pltpu.SemaphoreType.DMA((n_copy,)), pltpu.SemaphoreType.DMA((n_copy,)), pltpu.SemaphoreType.DMA((TWO,))],
        cost_estimate=pl.CostEstimate(flops=10**11, bytes_accessed=TWO**20, transcendentals=ZERO),
        compiler_params=pltpu.CompilerParams(vmem_limit_bytes=VMEM_LIMIT, collective_id=ZERO, has_side_effects=True),
    )(z_t[None], dy_t, mask_loc[None], w_in, w_out, w_gate, *vecs)
    da, keep, got, dgl, gram_o, dbg, dbo, dsc_o, dof_o, wg, sc_in, off_in, sv = outs[:13]

    args = (z_t, dy_t, mask_loc, da, keep, got, dgl, sv, wg, sc_in, off_in)
    const = lambda *shape: pl.BlockSpec(shape, lambda g: (ZERO,) * len(shape))
    dz_t, gram_i, dbias, dsc_i, dof_i = call(
        input_kernel, 'input_side', 42, *args, grid=(n_grp,),
        out_shape=(b16(rows, cz, cols), sds((cz, n_e * SUB), F32), sds((4 * ch, SUB, LANES), F32), sds((cz, cols), F32), sds((cz, cols), F32)),
        in_specs=[row3(cz), row3(cz), mask_spec, chan_rows(ch), chan_rows(half), chan_rows(half), chan_rows(cz),
                  pl.BlockSpec((4, ch, grp, cols), lambda g: (ZERO, ZERO, g, ZERO))] + [whole(x) for x in args[8:]],
        out_specs=(row3(cz), const(cz, n_e * SUB), const(4 * ch, SUB, LANES), const(cz, cols), const(cz, cols)),
        scratch_shapes=[pltpu.VMEM((n_e * SUB, cols), BF16)])

    n_sum = (-(3 * cz + SUB) // (n_dap * SUB)) * -SUB
    total = pl.pallas_call(
        functools.partial(sum_kernel, n_dap), name='weight_sums',
        out_shape=f32(n_sum * n_dap, LANES), in_specs=[vmem] * 9, out_specs=vmem,
        scratch_shapes=[pltpu.VMEM((n_sum * n_dap, LANES), F32), pltpu.VMEM((n_dap - ONE, n_sum, LANES), F32), pltpu.VMEM((n_sum, LANES), F32)]
        + [pltpu.SemaphoreType.DMA((n_dap - ONE,))] * 4,
        cost_estimate=pl.CostEstimate(flops=10**10, bytes_accessed=TWO**20, transcendentals=ZERO),
        compiler_params=pltpu.CompilerParams(vmem_limit_bytes=VMEM_LIMIT, collective_id=ONE, has_side_effects=True),
    )(gram_i, dbias, dsc_i, dof_i, gram_o, dsc_o, dof_o, dbo, dbg)
    row = lambda n: b16(ONE, n)
    grads = call(round_kernel, 'round', ONE, total,
                 out_shape=(row(cz), row(cz), b16(cz, 4 * ch), row(4 * ch), row(ch), row(ch), b16(ch, cz), row(cz), b16(cz, cz), row(cz)))
    grads = [g.reshape(-ONE) if g.shape[ZERO] == ONE else g for g in grads]
    return (jnp.transpose(dz_t, (ZERO, TWO, ONE)), *grads)


def solution(mesh):
    pair_spec = P(('batch', 'dap'), None, None)
    mask_spec = P(('batch', 'dap'), None)
    vec_rep = P(None)
    mat_rep = P(None, None)
    vec_part = P('batch')
    mat_part = P('batch', None)
    in_specs = (pair_spec, mask_spec, pair_spec, vec_rep, vec_rep, mat_rep, vec_rep, vec_rep, vec_rep, mat_rep, vec_rep, mat_rep, vec_rep)
    out_specs = (pair_spec, vec_part, vec_part, mat_part, vec_part, vec_part, vec_part, mat_part, vec_part, mat_part, vec_part)
    body = functools.partial(local_grads, mesh.shape['dap'])
    return jax.shard_map(body, mesh=mesh, in_specs=in_specs, out_specs=out_specs, check_vma=False)
```

```python
import functools
import jax
import jax.numpy as jnp
from jax import lax
from jax.experimental import pallas as pl
from jax.experimental.pallas import tpu as pltpu
from jax.sharding import PartitionSpec as P

LN_EPS = 1e-5
F32 = jnp.float32
BF16 = jnp.bfloat16
SUB = 8
VMEM_LIMIT = 63 * 1024 * 1024
COST = 5e8
ZERO, ONE, TWO = range(3)
LANES = 128


def nn_dot(lhs, rhs):
    return lax.dot_general(lhs, rhs, (((ONE,), (ZERO,)), ((), ())), preferred_element_type=F32)


def nt_dot(lhs, rhs):
    return lax.dot_general(lhs, rhs, (((ONE,), (ONE,)), ((), ())), preferred_element_type=F32)


def tn_dot(lhs, rhs):
    return lax.dot_general(lhs, rhs, (((ZERO,), (ZERO,)), ((), ())), preferred_element_type=F32)


def row_norm(z8, scale, offset):
    mean_val = jnp.mean(z8, axis=ONE, keepdims=True)
    centered = z8 - mean_val
    inv_std = lax.rsqrt(jnp.mean(centered * centered, axis=ONE, keepdims=True) + LN_EPS)
    z_hat = centered * inv_std
    return z_hat, inv_std, (z_hat * scale[None] + offset[None]).astype(BF16)


def lanes(bias, width):
    return jnp.concatenate([bias] * (width // bias.shape[-ONE]), axis=-ONE)


def gated(prod, bias_ref, start, chans, mask_half):
    cols = prod.shape[-ONE]
    val = prod[:chans * SUB].reshape(chans, SUB, cols) + lanes(bias_ref[start:start + chans], cols)
    gate = prod[chans * SUB:].reshape(chans, SUB, cols) + lanes(bias_ref[start + chans:start + TWO * chans], cols)
    return (jnp.tanh(gate) + 1.0) * (val * mask_half[None])


def build_weights(core, w_in, w_out, w_gate, vecs, wk_ref, wg_ref, bias_ref, sc_ref, off_ref, perm_s, wok_s, wotk_s, bo_s, osc_s, ooff_s):
    cz = w_in.shape[ZERO]
    ch = w_in.shape[ONE] // 4
    big = ch * SUB

    def iota(shape, dim):
        return lax.broadcasted_iota(jnp.int32, shape, dim)

    def one(cond):
        return jnp.where(cond, 1.0, 0.0).astype(BF16)

    turn = core * (ch // TWO)
    rep = iota((big, ch), ZERO) // SUB == iota((big, ch), ONE)
    rep_c = lax.rem(iota((big, ch), ZERO) // SUB + turn, ch) == iota((big, ch), ONE)
    rep_t = iota((ch, big), ONE) // SUB == iota((ch, big), ZERO)
    rep_ct = lax.rem(iota((ch, big), ONE) // SUB + turn, ch) == iota((ch, big), ZERO)
    tile = one(iota((cz, SUB * cz), ONE) % cz == iota((cz, SUB * cz), ZERO))
    tile_t = one(iota((SUB * cz, cz), ZERO) % cz == iota((SUB * cz, cz), ONE))
    keep = iota((big, SUB * cz), ZERO) % SUB == iota((big, SUB * cz), ONE) // cz
    keep_t = iota((SUB * cz, big), ONE) % SUB == iota((SUB * cz, big), ZERO) // cz
    same = iota((big, big), ZERO) % SUB == iota((big, big), ONE) % SUB

    def spread(wide):
        return jnp.where(keep, nn_dot(wide, tile), 0.0).astype(BF16)

    def column(sel, row, width):
        picked = jnp.where(sel, jnp.broadcast_to(row.astype(F32), sel.shape), 0.0).astype(BF16)
        return nn_dot(picked, jnp.ones((sel.shape[ONE], width), BF16))

    def eights(sel, row):
        return column(sel, row, LANES).reshape(ch, SUB, LANES)

    for dst, src, scale in ((ZERO, ZERO, 1.0), (ONE, TWO, 0.5), (TWO, ONE, 1.0), (3, 3, 0.5), (4, None, 1.0)):
        w_part = w_gate[...] if src is None else w_in[:, src * ch:(src + ONE) * ch]
        sel, sel_t = (rep, rep_t) if src is None else (rep_c, rep_ct)
        at = slice(dst * big, (dst + ONE) * big)
        wide = (nt_dot(one(sel), w_part) * scale).astype(BF16)
        wk_ref[at] = spread(wide)
        wg_ref[:, at] = jnp.where(keep_t, nn_dot(tile_t, nn_dot(w_part, one(sel_t)).astype(BF16)), 0.0).astype(BF16)
        vec = 5 if src is None else 6 + src
        bias_ref[dst * ch:(dst + ONE) * ch] = eights(sel, vecs[vec]) * scale
    eye = iota((cz, cz), ZERO) == iota((cz, cz), ONE)
    perm_s[...] = spread(one(rep))
    wok_s[...] = jnp.where(same, nn_dot(nt_dot(one(rep), w_out[...]).astype(BF16), one(rep_ct)), 0.0).astype(BF16)
    wotk_s[...] = jnp.where(same, nn_dot(nn_dot(one(rep_c), w_out[...]).astype(BF16), one(rep_t)), 0.0).astype(BF16)
    sc_ref[...] = column(eye, vecs[ZERO], sc_ref.shape[ONE])
    off_ref[...] = column(eye, vecs[ONE], off_ref.shape[ONE])
    osc_s[...] = eights(rep_c, vecs[TWO])
    ooff_s[...] = eights(rep_c, vecs[3])
    bo_s[...] = eights(rep, vecs[4])


def gate_parts(prod, bias_ref, start, chans):
    cols = prod.shape[-ONE]
    val = prod[:chans * SUB].reshape(chans, SUB, cols) + lanes(bias_ref[start:start + chans], cols)
    gate = prod[chans * SUB:].reshape(chans, SUB, cols) + lanes(bias_ref[start + chans:start + TWO * chans], cols)
    return val, jnp.tanh(gate) * 0.5 + 0.5


def project(z8, mask_half, wk_ref, bias_ref, sc_ref, off_ref, chans):
    cols = z8.shape[-ONE]
    _, _, zn = row_norm(z8.astype(F32), sc_ref[...], off_ref[...])
    zn2 = zn.reshape(SUB * zn.shape[ONE], cols)
    n_p = TWO * chans * SUB
    act_a = gated(nn_dot(wk_ref[:n_p], zn2), bias_ref, ZERO, chans, mask_half)
    act_b = gated(nn_dot(wk_ref[n_p:TWO * n_p], zn2), bias_ref, TWO * chans, chans, mask_half)
    return act_a, act_b, zn2


MESH = pl.DeviceIdType.MESH
OWN, LEFT, RIGHT, OPP = range(4)
HOPS = (ZERO, -ONE, ONE, TWO)


def blk(shape, index_map):
    return pl.BlockSpec(shape, index_map)


def front_kernel(n_dap, z_own, dy_ref, m_own, mask_in, w_in, w_out, w_gate, v_is, v_io, v_os, v_oo, v_bo, v_bg, v_bi,
                 da_ref, keep_ref, got_ref, dgl_ref, gram_ref, dbg_ref, dbo_ref, dsc_ref, dof_ref, wg_ref, sc_ref, off_ref,
                 sv_ref, give_ref, z_far, m_far, a_all, b_pair, a_sib, lg_ref, dyt_ref, do_out, do_in, relay, mask16,
                 wk_ref, bias_ref, perm_ref, wo_ref, wot_ref, bout_ref, osc_ref, ooff_ref,
                 o_s, gram_s, lg_v, dyt_v, do_v, dgl_v, mask_v, send_sem, recv_sem, loc_sem):
    n_chip = n_dap // TWO
    _, rows, cz, cols = z_own.shape
    z_ref = z_own.at[ZERO]
    chans = a_all.shape[ONE]
    half = chans // TWO
    hr = rows // TWO
    jb = TWO * rows
    grp = TWO * SUB
    me = lax.axis_index('dap')
    core, chip = lax.rem(me, TWO), me // TWO
    low = core == ZERO

    def peer(hop, flip):
        to = lax.rem(chip + (hop + n_chip), n_chip) * TWO
        return {'dap': to + (ONE - core if flip else core)}

    def copy(k, src, dst, hop, flip):
        return pltpu.make_async_remote_copy(src_ref=src, dst_ref=dst, send_sem=send_sem.at[k], recv_sem=recv_sem.at[k],
                                            device_id=peer(hop, flip), device_id_type=MESH)

    barrier = pltpu.get_barrier_semaphore()
    for hop in HOPS:
        for flip in (ZERO, ONE):
            if hop or flip:
                pl.semaphore_signal(barrier, inc=ONE, device_id=peer(hop, flip), device_id_type=MESH)
    pl.semaphore_wait(barrier, n_dap - ONE)

    n_grp = rows // grp
    masks = [copy(i, mask16, m_far.at[i], hop, ZERO) for i, hop in enumerate((ONE, -ONE, TWO))]
    quarter = lambda q: pl.ds(pl.multiple_of(q * grp, grp), grp)
    z_r = lambda q: copy(3 + q, z_ref.at[quarter(q)], z_far.at[ZERO, quarter(q)], ONE, ZERO)
    z_l = lambda q: copy(3 + n_grp + q, z_ref.at[quarter(q)], z_far.at[ONE, quarter(q)], -ONE, ZERO)
    fwd_r = lambda q: copy(3 + TWO * n_grp + q, z_far.at[ZERO, quarter(q)], z_far.at[TWO, quarter(q)], ONE, ZERO)
    fwd_l = lambda q: copy(3 + TWO * n_grp + q, z_far.at[ONE, quarter(q)], z_far.at[TWO, quarter(q)], -ONE, ZERO)
    base_b = 3 + 3 * n_grp
    my_rows = pl.multiple_of(core * rows, rows)

    def swap_b(r, q):
        at = pl.ds(pl.multiple_of(my_rows + q * grp, grp), grp)
        return [copy(base_b + (r * n_grp + q) * TWO + h, b_pair.at[r, pl.ds(h * half, half), at], b_pair.at[r, pl.ds((ONE - h) * half, half), at], ZERO, ONE) for h in (ZERO, ONE)]

    base_a = base_b + 8 * n_grp
    swap_a = lambda r, q: copy(base_a + r * n_grp + q, a_all.at[r, pl.ds(half, half), quarter(q)], a_sib.at[r, :, quarter(q)], ZERO, ONE)
    base_s = base_a + 4 * n_grp
    back = (OWN, RIGHT, LEFT, OPP)
    ship = [[None if (r == OWN and side == ZERO) else
             copy(base_s + TWO * r + side, do_out.at[r, pl.ds(side * half, half)], do_in.at[back[r], side], HOPS[r], side) for side in (ZERO, ONE)] for r in range(4)]
    onward = []
    swap_d = [copy(base_s + 8 + q, give_ref.at[pl.ds(q * (half // TWO), half // TWO)], got_ref.at[pl.ds(q * (half // TWO), half // TWO)], ZERO, ONE) for q in (ZERO, ONE)]

    for q in range(n_grp):
        z_r(q).start()
        z_l(n_grp - ONE - q).start()
        if q == ZERO:
            mask_v[...] = mask_in[...].astype(BF16)
            put = pltpu.make_async_copy(mask_v, mask16, loc_sem.at[ZERO])
            put.start()
            put.wait()
            for c in masks:
                c.start()
    b_all = v_bi[...]
    vecs = [ref[...] for ref in (v_is, v_io, v_os, v_oo, v_bo, v_bg)] + [b_all[:, i * chans:(i + ONE) * chans] for i in range(4)]
    build_weights(core, w_in, w_out, w_gate, vecs, wk_ref, wg_ref, bias_ref, sc_ref, off_ref, perm_ref, wo_ref, wot_ref, bout_ref, osc_ref, ooff_ref)

    row3 = blk((grp, cz, cols), lambda g: (g, ZERO, ZERO))
    row2 = blk((grp, cols), lambda g: (g, ZERO))
    chan3 = lambda n: blk((n, grp, cols), lambda g: (ZERO, g, ZERO))

    def ab_body(z_b, m_b, a_b, b_b):
        a_parts, b_parts = [], []
        for h in range(TWO):
            rws = slice(h * SUB, (h + ONE) * SUB)
            act_a, act_b, _ = project(z_b[ZERO, rws], m_b[ZERO].astype(F32)[rws] * 0.5, wk_ref, bias_ref, sc_ref, off_ref, chans)
            a_parts.append(act_a)
            b_parts.append(act_b)
        a_b[ZERO] = jnp.concatenate(a_parts, axis=ONE).astype(BF16)
        b_b[ZERO] = jnp.concatenate(b_parts, axis=ONE).astype(BF16)

    def own_body(z_b, m_b, a_b, b_b, sv_b):
        acts = ([], [])
        for h in range(TWO):
            rws = slice(h * SUB, (h + ONE) * SUB)
            _, _, zn = row_norm(z_b[ZERO, rws].astype(F32), sc_ref[...], off_ref[...])
            zn2 = zn.reshape(SUB * cz, cols)
            mask = m_b[ZERO, rws].astype(F32)[None]
            n_p = TWO * chans * SUB
            for side in (ZERO, ONE):
                val, sig = gate_parts(nn_dot(wk_ref[side * n_p:(side + ONE) * n_p], zn2), bias_ref, TWO * side * chans, chans)
                sv_b[TWO * side, :, rws] = val
                sv_b[TWO * side + ONE, :, rws] = sig
                acts[side].append(mask * sig * val)
        a_b[ZERO] = jnp.concatenate(acts[ZERO], axis=ONE).astype(BF16)
        b_b[ZERO] = jnp.concatenate(acts[ONE], axis=ONE).astype(BF16)

    def project_rows(z_src, m_src, n, slot, place):
        pltpu.emit_pipeline(
            ab_body, grid=(n,),
            in_specs=[blk((ONE, grp, cz, cols), lambda g: (slot(g), place(g)[ONE], ZERO, ZERO)), blk((ONE, grp, cols), lambda g: (slot(g), place(g)[ONE], ZERO))],
            out_specs=[blk((ONE, chans, grp, cols), lambda g: (place(g)[ZERO], ZERO, place(g)[ONE], ZERO)),
                       blk((ONE, chans, grp, cols), lambda g: (place(g)[ZERO], ZERO, core * n_grp + place(g)[ONE], ZERO))])(z_src, m_src, a_all, b_pair)

    def swap(r, q):
        for c in swap_b(r, q):
            c.start()
        swap_a(r, q).start()

    def swapped_b(r):
        def body(q, carry):
            for c in swap_b(r, q):
                c.wait_recv()
            return carry
        lax.fori_loop(ZERO, n_grp, body, ZERO)

    def lg_body(z_b, dy_b, lg_b, dyt_b):
        dy_parts = []
        for h in range(TWO):
            rws = slice(h * SUB, (h + ONE) * SUB)
            _, _, zn = row_norm(z_b[rws].astype(F32), sc_ref[...], off_ref[...])
            zn2 = zn.reshape(SUB * cz, cols)
            lg_b[:, rws, :] = nn_dot(wk_ref[4 * chans * SUB:], zn2).reshape(cz, SUB, cols) + lanes(bias_ref[4 * chans:], cols)
            dy_parts.append(nn_dot(perm_ref[...], dy_b[rws].reshape(SUB * cz, cols)).reshape(cz, SUB, cols))
        dyt_b[...] = jnp.concatenate(dy_parts, axis=ONE).astype(BF16)

    for ref in (dbg_ref, dbo_ref, dsc_ref, dof_ref, gram_s):
        ref[...] = jnp.zeros_like(ref)

    per = chans // 8

    def o_body(a_b, b_b):
        base = pl.program_id(ZERO) * per
        for c in range(ZERO, per, TWO):
            both = nt_dot(a_b[c:c + TWO].reshape(TWO * rows, cols), b_b[c:c + TWO].reshape(TWO * jb, cols))
            o_s[base + c] = both[:rows, :jb]
            o_s[base + c + ONE] = both[rows:, jb:]

    def chain(r):
        where = lax.rem(chip + (HOPS[r] + n_chip), n_chip)
        col = pl.ds(pl.multiple_of(where * jb, jb), jb)
        get_lg = pltpu.make_async_copy(lg_ref.at[:, :, col], lg_v, loc_sem.at[ZERO])
        get_dy = pltpu.make_async_copy(dyt_ref.at[:, :, col], dyt_v, loc_sem.at[ONE])
        get_lg.start()
        get_dy.start()
        pltpu.emit_pipeline(o_body, grid=(8,), in_specs=[blk((per, rows, cols), lambda s: (s, ZERO, ZERO)), blk((per, jb, cols), lambda s: (s, ZERO, ZERO))])(
            a_all.at[OWN], b_pair.at[r])
        get_lg.wait()
        get_dy.wait()

        def chain_body(g, carry):
            pair = pl.ds(pl.multiple_of(g * TWO * SUB, TWO * SUB), TWO * SUB)

            def wide(ref):
                val = ref[:, pair, :].astype(F32)
                return jnp.concatenate([val[:, :SUB], val[:, SUB:]], axis=TWO)

            def tall(val):
                return jnp.concatenate([val[..., :jb], val[..., jb:]], axis=ONE)

            def add(ref, val):
                ref[...] += val[..., :jb] + val[..., jb:]

            twice = lambda ref: lanes(ref[...], TWO * jb)
            o8 = wide(o_s)
            centered = o8 - jnp.mean(o8, axis=ZERO, keepdims=True)
            inv_std = lax.rsqrt(jnp.mean(centered * centered, axis=ZERO, keepdims=True) + LN_EPS)
            o_hat = centered * inv_std
            o_norm = (o_hat * twice(osc_ref) + twice(ooff_ref)).astype(BF16).reshape(chans * SUB, TWO * jb)
            upd = (nn_dot(wo_ref[...], o_norm).reshape(cz, SUB, TWO * jb) + twice(bout_ref)).astype(BF16).astype(F32)
            sig = jnp.tanh(wide(lg_v) * 0.5) * 0.5 + 0.5
            prod = sig * wide(dyt_v)
            d_upd = prod.astype(BF16)
            dgl = prod * upd * (1.0 - sig)
            add(dbg_ref, dgl)
            dgl_v[:, pair, :] = tall(dgl).astype(BF16)
            add(dbo_ref, d_upd.astype(F32))
            d_upd2 = d_upd.reshape(cz * SUB, TWO * jb)
            gram_s[...] += nt_dot(o_norm, d_upd2)
            d_on = nn_dot(wot_ref[...], d_upd2).astype(BF16).astype(F32).reshape(chans, SUB, TWO * jb)
            add(dsc_ref, d_on * o_hat)
            add(dof_ref, d_on)
            g_hat = d_on * twice(osc_ref)
            m1 = jnp.mean(g_hat, axis=ZERO, keepdims=True)
            m2 = jnp.mean(g_hat * o_hat, axis=ZERO, keepdims=True)
            do_v[:, pair, :] = tall(inv_std * (g_hat - m1 - o_hat * m2)).astype(BF16)
            return carry
        lax.fori_loop(ZERO, rows // (TWO * SUB), chain_body, ZERO)
        put_do = pltpu.make_async_copy(do_v, do_out.at[r], loc_sem.at[ZERO])
        put_gl = pltpu.make_async_copy(dgl_v, dgl_ref.at[:, :, col], loc_sem.at[ONE])
        put_do.start()
        put_gl.start()
        put_do.wait()
        put_gl.wait()
        for c in ship[r]:
            if c is not None:
                c.start()

    pltpu.emit_pipeline(
        own_body, grid=(n_grp,),
        in_specs=[blk((ONE, grp, cz, cols), lambda g: (ZERO, g, ZERO, ZERO)), blk((ONE, grp, cols), lambda g: (ZERO, g, ZERO))],
        out_specs=[blk((ONE, chans, grp, cols), lambda g: (OWN, ZERO, g, ZERO)), blk((ONE, chans, grp, cols), lambda g: (OWN, ZERO, core * n_grp + g, ZERO)),
                   blk((4, chans, grp, cols), lambda g: (ZERO, ZERO, g, ZERO))])(z_own, m_own, a_all, b_pair, sv_ref)
    for q in range(n_grp):
        swap(OWN, q)
    pltpu.emit_pipeline(lg_body, grid=(n_grp,), in_specs=[row3, row3], out_specs=[chan3(cz), chan3(cz)])(z_own.at[ZERO], dy_ref, lg_ref, dyt_ref)
    swapped_b(OWN)
    chain(OWN)
    for c in masks:
        c.wait_recv()

    def sides(t, carry):
        z_r(t).wait_recv()
        z_l(n_grp - ONE - t).wait_recv()

        @pl.when(t < n_grp // TWO)
        def _():
            fwd_r(t).start()
            fwd_l(n_grp - ONE - t).start()
        project_rows(z_far, m_far, TWO, lambda g: g, lambda g: (g + LEFT, jnp.where(g == ZERO, t, n_grp - ONE - t)))
        swap(LEFT, t)
        swap(RIGHT, n_grp - ONE - t)
        return carry
    lax.fori_loop(ZERO, n_grp, sides, ZERO)
    swapped_b(LEFT)
    chain(LEFT)
    swapped_b(RIGHT)
    chain(RIGHT)

    def opposite(t, carry):
        fwd_r(t).wait_recv()
        fwd_l(n_grp - ONE - t).wait_recv()
        project_rows(z_far, m_far, TWO, lambda g: TWO, lambda g: (OPP, jnp.where(g == ZERO, t, n_grp - ONE - t)))
        swap(OPP, t)
        swap(OPP, n_grp - ONE - t)
        return carry
    lax.fori_loop(ZERO, n_grp // TWO, opposite, ZERO)
    swapped_b(OPP)
    chain(OPP)

    gram = gram_s[...]
    n = gram.shape[ZERO]
    diag = lax.broadcasted_iota(jnp.int32, (n, n), ZERO) % SUB == lax.broadcasted_iota(jnp.int32, (n, n), ONE) % SUB
    gram_ref[...] = jnp.sum(jnp.where(diag, gram, 0.0).reshape(chans, SUB, n), axis=ONE)

    pc = 8
    n_a = chans // pc

    def da_body(do_b, b_b, da_b):
        for c in range(da_b.shape[ZERO]):
            lhs = jnp.concatenate([do_b[r, c] for r in range(4)], axis=ONE)
            rhs = jnp.concatenate([b_b[r, c] for r in range(4)], axis=ZERO)
            da_b[c] = nn_dot(lhs, rhs).astype(BF16)

    pltpu.emit_pipeline(
        da_body, grid=(n_a,),
        in_specs=[blk((4, pc, rows, jb), lambda s: (ZERO, s, ZERO, ZERO)), blk((4, pc, jb, cols), lambda s: (ZERO, s, ZERO, ZERO))],
        out_specs=[blk((pc, rows, cols), lambda s: (s, ZERO, ZERO))])(do_out, b_pair, da_ref)

    pc = 8
    for r in range(4):
        lax.fori_loop(ZERO, n_grp, lambda q, carry, r=r: (swap_a(r, q).wait_recv(), carry)[ONE], ZERO)
        for c in ship[r]:
            if c is not None:
                c.wait_recv()

    def db_body(own_b, do0_b, do1_b, am_b, as_b, keep_b, give_b):
        for c in range(pc):
            lhs, rhs = [], []
            for r in range(4):
                lhs += [own_b[ZERO, c] if r == OWN else do0_b[r - ONE, c], do1_b[r, ZERO, c]]
                rhs += [am_b[r, c], as_b[r, c]]
            pair = tn_dot(jnp.concatenate(lhs, axis=ZERO), jnp.concatenate(rhs, axis=ZERO)).astype(BF16)
            keep_b[c] = jnp.where(low, pair[:rows], pair[rows:])
            give_b[c] = jnp.where(low, pair[rows:], pair[:rows])

    for q in (ZERO, ONE):
        steps = half // pc // TWO
        at = lambda s: s + q * steps
        c3 = blk((pc, rows, cols), lambda s: (at(s), ZERO, ZERO))
        pltpu.emit_pipeline(
            db_body, grid=(steps,),
            in_specs=[blk((ONE, pc, rows, jb), lambda s: (ZERO, at(s), ZERO, ZERO)), blk((3, pc, rows, jb), lambda s: (ZERO, at(s), ZERO, ZERO)),
                      blk((4, ONE, pc, rows, jb), lambda s: (ZERO, ZERO, at(s), ZERO, ZERO)),
                      c4_at(pc, rows, cols, at), c4_at(pc, rows, cols, at)],
            out_specs=[c3, c3])(do_out, do_in.at[pl.ds(ONE, 3), ZERO], do_in.at[:, pl.ds(ONE, ONE)], a_all, a_sib, keep_ref, give_ref)
        swap_d[q].start()
    for c in swap_d:
        c.wait_recv()
    for c in masks + swap_d + onward + [c for pair in ship for c in pair if c is not None]:
        c.wait_send()

    def sent(q, carry):
        z_r(q).wait_send()
        z_l(q).wait_send()
        for r in range(4):
            for c in swap_b(r, q) + [swap_a(r, q)]:
                c.wait_send()

        @pl.when(q < n_grp // TWO)
        def _():
            fwd_r(q).wait_send()

        @pl.when(q >= n_grp // TWO)
        def _():
            fwd_l(q).wait_send()
        return carry
    lax.fori_loop(ZERO, n_grp, sent, ZERO)


def c4_at(pc, rows, cols, at):
    return pl.BlockSpec((4, pc, rows, cols), lambda s: (ZERO, at(s), ZERO, ZERO))


def input_kernel(z_ref, dy_ref, mask_ref, da_ref, db0_ref, db1_ref, dgl_ref, sv_ref, wg_ref, sc_ref, off_ref,
                 dz_ref, gram_ref, dbias_ref, dsc_ref, dof_ref, dp_s):
    chans = da_ref.shape[ZERO]
    chan_z, cols = z_ref.shape[ONE:]

    @pl.when(pl.program_id(ZERO) == ZERO)
    def _():
        for ref in (gram_ref, dbias_ref, dsc_ref, dof_ref):
            ref[...] = jnp.zeros_like(ref)

    def fold(val):
        acc = val[..., :LANES]
        for lane in range(LANES, cols, LANES):
            acc = acc + val[..., lane:lane + LANES]
        return acc

    n_p = chans * SUB
    grads = (da_ref[...].astype(F32), jnp.concatenate([db0_ref[...], db1_ref[...]], axis=ZERO).astype(F32))
    for half in range(TWO):
        rows = slice(half * SUB, (half + ONE) * SUB)
        z_hat, inv_std, zn = row_norm(z_ref[rows].astype(F32), sc_ref[...], off_ref[...])
        zn2 = zn.reshape(SUB * chan_z, cols)
        mask_f = mask_ref[rows].astype(F32)[None]
        for side, grad_all in enumerate(grads):
            val, sig = sv_ref[TWO * side, :, rows], sv_ref[TWO * side + ONE, :, rows]
            grad = grad_all[:, rows] * mask_f
            d_val = grad * sig
            d_gate = d_val * val * (1.0 - sig)
            dbias_ref[TWO * side * chans:(TWO * side + ONE) * chans] += fold(d_val)
            dbias_ref[(TWO * side + ONE) * chans:(TWO * side + TWO) * chans] += fold(d_gate)
            dp_s[TWO * side * n_p:(TWO * side + ONE) * n_p] = d_val.astype(BF16).reshape(n_p, cols)
            dp_s[(TWO * side + ONE) * n_p:(TWO * side + TWO) * n_p] = d_gate.astype(BF16).reshape(n_p, cols)
        dp_s[4 * n_p:] = dgl_ref[...].astype(F32)[:, rows].astype(BF16).reshape(n_p, cols)
        d_zn = nn_dot(wg_ref[...], dp_s[...]).astype(BF16).astype(F32).reshape(SUB, chan_z, cols)
        gram = nt_dot(zn2, dp_s[...]).reshape(SUB, chan_z, dp_s.shape[ZERO])
        lane_row = lax.broadcasted_iota(jnp.int32, (chan_z, dp_s.shape[ZERO]), ONE) % SUB
        acc = gram_ref[...]
        for i in range(SUB):
            acc = acc + jnp.where(lane_row == i, gram[i], 0.0)
        gram_ref[...] = acc
        dsc_ref[...] += jnp.sum(d_zn * z_hat, axis=ZERO)
        dof_ref[...] += jnp.sum(d_zn, axis=ZERO)
        g_hat = d_zn * sc_ref[...][None]
        m1 = jnp.mean(g_hat, axis=ONE, keepdims=True)
        m2 = jnp.mean(g_hat * z_hat, axis=ONE, keepdims=True)
        d_z = dy_ref[rows].astype(F32) + inv_std * (g_hat - m1 - z_hat * m2)
        dz_ref[rows] = d_z.astype(BF16)


def exact_dot(lhs, rhs, dims):
    return lax.dot_general(lhs, rhs, (dims, ((), ())), precision=lax.Precision.HIGHEST, preferred_element_type=F32)


def sum_kernel(n_dap, gram_i, dbias, dsc_i, dof_i, gram_o, dsc_o, dof_o, dbo, dbg, out_ref, part_s, in_s, mine_s, send_sem, recv_sem, send2, recv2):
    me = lax.axis_index('dap')
    core = lax.rem(me, TWO)
    low = core == ZERO
    barrier = pltpu.get_barrier_semaphore()
    to = [lax.rem(me + d, n_dap) for d in range(n_dap)]
    for d in range(ONE, n_dap):
        pl.semaphore_signal(barrier, inc=ONE, device_id={'dap': to[d]}, device_id_type=MESH)
    cz = gram_i.shape[ZERO]
    ch = gram_o.shape[ZERO]
    big = ch * SUB
    turn = core * (ch // TWO)
    row = lax.broadcasted_iota(jnp.int32, (big, ch), ZERO) // SUB
    col = lax.broadcasted_iota(jnp.int32, (big, ch), ONE)
    fold = jnp.where(row == col, 1.0, 0.0)
    fold_c = jnp.where(lax.rem(row + turn, ch) == col, 1.0, 0.0)
    part_s[...] = jnp.zeros_like(part_s)
    for dst, src in ((ZERO, ZERO), (ONE, TWO), (TWO, ONE), (3, 3), (4, 4)):
        val = exact_dot(gram_i[:, dst * big:(dst + ONE) * big], fold if src == 4 else fold_c, ((ONE,), (ZERO,)))
        part_s[(src // TWO) * cz:(src // TWO + ONE) * cz, (src % TWO) * ch:(src % TWO + ONE) * ch] = val
    val = exact_dot(gram_o[...], fold, ((ONE,), (ZERO,)))
    h = ch // TWO
    val = jnp.where(low, val, jnp.concatenate([val[h:], val[:h]], axis=ZERO))
    part_s[TWO * cz:3 * cz, ch:TWO * ch] = val
    eye = lax.broadcasted_iota(jnp.int32, (ch, ch), ZERO)
    lane = lax.broadcasted_iota(jnp.int32, (ch, ch), ONE)
    order = jnp.where(lax.rem(eye + turn, ch) == lane, 1.0, 0.0)

    def line(acc, ordered):
        flat = jnp.sum(acc, axis=ONE) if len(acc.shape) == 3 else acc
        res = exact_dot(jnp.ones((SUB, flat.shape[ONE]), F32), flat, ((ONE,), (ONE,)))
        return exact_dot(res, order, ((ONE,), (ZERO,)))[:ONE] if ordered else res[:ONE]

    base = 3 * cz
    for dst, src in ((ZERO, ZERO), (ONE, TWO), (TWO, ONE), (3, 3)):
        part_s[base + src // TWO:base + src // TWO + ONE, (src % TWO) * ch:(src % TWO + ONE) * ch] = line(dbias[dst * ch:(dst + ONE) * ch], True)
    part_s[base + TWO:base + 3, :ch] = line(dsc_i[...], False)
    part_s[base + TWO:base + 3, ch:TWO * ch] = line(dof_i[...], False)
    part_s[base + 3:base + 4, :ch] = line(dsc_o[...], True)
    part_s[base + 3:base + 4, ch:TWO * ch] = line(dof_o[...], True)
    part_s[base + 4:base + 5, :ch] = line(dbo[...], False)
    part_s[base + 4:base + 5, ch:TWO * ch] = line(dbg[...], False)

    pl.semaphore_wait(barrier, n_dap - ONE)
    n = mine_s.shape[ZERO]

    def scatter(d):
        return pltpu.make_async_remote_copy(src_ref=part_s.at[pl.ds(pl.multiple_of(to[d] * n, n), n)], dst_ref=in_s.at[d - ONE],
                                            send_sem=send_sem.at[d - ONE], recv_sem=recv_sem.at[d - ONE],
                                            device_id={'dap': to[d]}, device_id_type=MESH)

    at = pl.ds(pl.multiple_of(me * n, n), n)

    def spread(d):
        return pltpu.make_async_remote_copy(src_ref=mine_s, dst_ref=out_ref.at[at], send_sem=send2.at[d - ONE], recv_sem=recv2.at[d - ONE],
                                            device_id={'dap': to[d]}, device_id_type=MESH)

    for d in range(ONE, n_dap):
        scatter(d).start()
    total = part_s[at]
    for d in range(ONE, n_dap):
        scatter(d).wait_recv()
        total = total + in_s[d - ONE]
    mine_s[...] = total
    for d in range(ONE, n_dap):
        spread(d).start()
    out_ref[at] = total
    for d in range(ONE, n_dap):
        spread(d).wait_recv()
    for d in range(ONE, n_dap):
        scatter(d).wait_send()
        spread(d).wait_send()


def round_kernel(tot_ref, sc_ref, off_ref, w_ref, b_ref, osc_ref, ooff_ref, wout_ref, bout_ref, wg_ref, bg_ref):
    cz, ch = wg_ref.shape
    tot = tot_ref[...].astype(BF16)
    base = 3 * cz
    w_ref[:, :TWO * ch] = tot[:cz]
    w_ref[:, TWO * ch:] = tot[cz:TWO * cz]
    wg_ref[...] = tot[TWO * cz:3 * cz, :ch]
    wout_ref[...] = tot[TWO * cz:3 * cz, ch:]
    vec = tot_ref[base:base + SUB]
    for ref, r, c in ((b_ref, ZERO, ZERO), (sc_ref, TWO, ZERO), (off_ref, TWO, ONE), (osc_ref, 3, ZERO), (ooff_ref, 3, ONE), (bout_ref, 4, ZERO), (bg_ref, 4, ONE)):
        if ref is b_ref:
            ref[:, :TWO * ch] = vec[ZERO:ONE].astype(BF16)
            ref[:, TWO * ch:] = vec[ONE:TWO].astype(BF16)
        else:
            ref[...] = vec[r:r + ONE, c * ch:(c + ONE) * ch].astype(BF16)


def whole(arr):
    nd = arr.ndim
    return pl.BlockSpec(arr.shape, lambda *_: (ZERO,) * nd, pipeline_mode=pl.Buffered(ONE))


def call(kernel, name, us, *args, **kw):
    cost = pl.CostEstimate(flops=int(us * COST), bytes_accessed=TWO**20, transcendentals=ZERO)
    return pl.pallas_call(kernel, name=name, cost_estimate=cost, compiler_params=pltpu.CompilerParams(vmem_limit_bytes=VMEM_LIMIT), **kw)(*args)


def local_grads(n_dap, z_loc, mask_loc, dy_loc, ln_in_scale, ln_in_offset, w_in, b_in, ln_out_scale, ln_out_offset, w_out, b_out, w_gate, b_gate):
    rows, cols, cz = z_loc.shape
    ch = w_in.shape[ONE] // 4
    half = ch // TWO
    jb = TWO * rows
    grp = TWO * SUB
    n_grp = rows // grp
    sds = jax.ShapeDtypeStruct
    z_t = jnp.transpose(z_loc, (ZERO, TWO, ONE))
    dy_t = jnp.transpose(dy_loc, (ZERO, TWO, ONE))

    n_e = 5 * ch
    b16 = lambda *shape: sds(shape, BF16)
    vecs = [v.reshape(ONE, -ONE) for v in (ln_in_scale, ln_in_offset, ln_out_scale, ln_out_offset, b_out, b_gate, b_in)]
    row3 = lambda nd: pl.BlockSpec((grp, nd, cols), lambda g: (g, ZERO, ZERO))
    chan_rows = lambda n: pl.BlockSpec((n, grp, cols), lambda g: (ZERO, g, ZERO))
    mask_spec = pl.BlockSpec((grp, cols), lambda g: (g, ZERO))
    f32 = lambda *shape: sds(shape, F32)
    any_spec = pl.BlockSpec(memory_space=pl.ANY)
    vmem = pl.BlockSpec(memory_space=pltpu.VMEM)
    n_copy = 15 + 15 * n_grp
    acc = f32(ch, SUB, LANES)
    blocks = pltpu.VMEM((ch * SUB, cz * SUB), BF16)
    spread = pltpu.VMEM((ch, SUB, LANES), F32)
    outs = pl.pallas_call(
        functools.partial(front_kernel, n_dap), name='front',
        out_shape=(b16(ch, rows, cols), b16(half, rows, cols), b16(half, rows, cols), b16(cz, rows, cols), f32(ch, cz * SUB), acc, acc, acc, acc,
                   b16(SUB * cz, n_e * SUB), f32(cz, cols), f32(cz, cols),
                   f32(4, ch, rows, cols), b16(half, rows, cols), b16(3, rows, cz, cols), b16(3, rows, cols), b16(4, ch, rows, cols), b16(4, ch, jb, cols),
                   b16(4, half, rows, cols), f32(cz, rows, cols), b16(cz, rows, cols), b16(4, ch, rows, jb), b16(4, TWO, half, rows, jb), b16(TWO, half, rows, jb), b16(rows, cols)),
        in_specs=[any_spec] * 3 + [vmem] * 11,
        out_specs=(any_spec,) * 4 + (vmem,) * 8 + (any_spec,) * 13,
        scratch_shapes=[pltpu.VMEM((n_e * SUB, SUB * cz), BF16), pltpu.VMEM((n_e, SUB, LANES), F32), blocks, blocks, blocks, spread, spread, spread,
                        pltpu.VMEM((ch, rows, jb), F32), pltpu.VMEM((ch * SUB, cz * SUB), F32), pltpu.VMEM((cz, rows, jb), F32),
                        pltpu.VMEM((cz, rows, jb), BF16), pltpu.VMEM((ch, rows, jb), BF16), pltpu.VMEM((cz, rows, jb), BF16),
                        pltpu.VMEM((rows, cols), BF16),
                        pltpu.SemaphoreType.DMA((n_copy,)), pltpu.SemaphoreType.DMA((n_copy,)), pltpu.SemaphoreType.DMA((TWO,))],
        cost_estimate=pl.CostEstimate(flops=10**11, bytes_accessed=TWO**20, transcendentals=ZERO),
        compiler_params=pltpu.CompilerParams(vmem_limit_bytes=VMEM_LIMIT, collective_id=ZERO, has_side_effects=True),
    )(z_t[None], dy_t, mask_loc[None], mask_loc, w_in, w_out, w_gate, *vecs)
    da, keep, got, dgl, gram_o, dbg, dbo, dsc_o, dof_o, wg, sc_in, off_in, sv = outs[:13]

    args = (z_t, dy_t, mask_loc, da, keep, got, dgl, sv, wg, sc_in, off_in)
    const = lambda *shape: pl.BlockSpec(shape, lambda g: (ZERO,) * len(shape))
    dz_t, gram_i, dbias, dsc_i, dof_i = call(
        input_kernel, 'input_side', 42, *args, grid=(n_grp,),
        out_shape=(b16(rows, cz, cols), sds((cz, n_e * SUB), F32), sds((4 * ch, SUB, LANES), F32), sds((cz, cols), F32), sds((cz, cols), F32)),
        in_specs=[row3(cz), row3(cz), mask_spec, chan_rows(ch), chan_rows(half), chan_rows(half), chan_rows(cz),
                  pl.BlockSpec((4, ch, grp, cols), lambda g: (ZERO, ZERO, g, ZERO))] + [whole(x) for x in args[8:]],
        out_specs=(row3(cz), const(cz, n_e * SUB), const(4 * ch, SUB, LANES), const(cz, cols), const(cz, cols)),
        scratch_shapes=[pltpu.VMEM((n_e * SUB, cols), BF16)])

    n_sum = (-(3 * cz + SUB) // (n_dap * SUB)) * -SUB
    total = pl.pallas_call(
        functools.partial(sum_kernel, n_dap), name='weight_sums',
        out_shape=f32(n_sum * n_dap, LANES), in_specs=[vmem] * 9, out_specs=vmem,
        scratch_shapes=[pltpu.VMEM((n_sum * n_dap, LANES), F32), pltpu.VMEM((n_dap - ONE, n_sum, LANES), F32), pltpu.VMEM((n_sum, LANES), F32)]
        + [pltpu.SemaphoreType.DMA((n_dap - ONE,))] * 4,
        cost_estimate=pl.CostEstimate(flops=10**10, bytes_accessed=TWO**20, transcendentals=ZERO),
        compiler_params=pltpu.CompilerParams(vmem_limit_bytes=VMEM_LIMIT, collective_id=ONE, has_side_effects=True),
    )(gram_i, dbias, dsc_i, dof_i, gram_o, dsc_o, dof_o, dbo, dbg)
    row = lambda n: b16(ONE, n)
    grads = call(round_kernel, 'round', ONE, total,
                 out_shape=(row(cz), row(cz), b16(cz, 4 * ch), row(4 * ch), row(ch), row(ch), b16(ch, cz), row(cz), b16(cz, cz), row(cz)))
    grads = [g.reshape(-ONE) if g.shape[ZERO] == ONE else g for g in grads]
    return (jnp.transpose(dz_t, (ZERO, TWO, ONE)), *grads)


def solution(mesh):
    pair_spec = P(('batch', 'dap'), None, None)
    mask_spec = P(('batch', 'dap'), None)
    vec_rep = P(None)
    mat_rep = P(None, None)
    vec_part = P('batch')
    mat_part = P('batch', None)
    in_specs = (pair_spec, mask_spec, pair_spec, vec_rep, vec_rep, mat_rep, vec_rep, vec_rep, vec_rep, mat_rep, vec_rep, mat_rep, vec_rep)
    out_specs = (pair_spec, vec_part, vec_part, mat_part, vec_part, vec_part, vec_part, mat_part, vec_part, mat_part, vec_part)
    body = functools.partial(local_grads, mesh.shape['dap'])
    return jax.shard_map(body, mesh=mesh, in_specs=in_specs, out_specs=out_specs, check_vma=False)
```
